128 devices in a mesh: row: 32 (over z, x, core), col: 4 (over y).
Axes of the slice: x: 4, y: 4, z: 4, core: 2. Of those that a mesh axis runs over, the one named last changes fastest.
Arguments:
- prior_scores: float32 [12288, 12288], P('row', 'col'), may hold values from 0.001 to 10
- tiles_first: bfloat16 [96, 5, 128, 128], P('row'), may hold values from 0 to 1, as said below
- columns_first: int32 [96, 5], P('row'), may hold values from 0 to 95, as said below
- tiles_second: bfloat16 [96, 5, 128, 128], P('col'), may hold values from 0 to 1, as said below
- columns_second: int32 [96, 5], P('col'), may hold values from 0 to 95, as said below
Outputs:
- alignment: float32 [12288, 12288], P('row', 'col')
The draws below stay inside these ranges and needn't reach their ends.
Inputs may be any that keep to these rules, and one draw needn't show every extreme that they name: `tiles_first`: in every block row, the block in the first slot has entries of 0.5 or more on its diagonal. `tiles_second`: in every block row, the block in the first slot has entries of 0.5 or more on its diagonal. `columns_first`: each block row lists 5 different block columns. `columns_second`: each block row lists 5 different block columns.
All inputs are finite; a program needn't handle non-finite values.
Results may differ from the reference program's by a relative error of at most 0.0004.
The reference program's roundings to bfloat16 on the way count: a program that leaves them out, or rounds other values in their place, can miss the bound.
Values may be sent and summed in bfloat16 or wider, within the bound.
A program may use at most 192 MiB of HBM per device.

```python
import jax
import jax.numpy as jnp
from jax import lax

NODES_A = 12288
NODES_B = 12288
TILE = 128
SLOTS = 5
ITERS = 2


weight_span = 13.815510557964274


log_ten = 2.302585092994046


def tile_draw(key, block_count):
    tile_shape = (block_count, SLOTS, TILE, TILE)
    keep_key, level_key, extra_key, diagonal_key = jax.random.split(key, 4)
    kept_mask = jax.random.randint(keep_key, tile_shape, 0, 3) == 0
    level_draw = jax.random.uniform(level_key, tile_shape, dtype=jnp.float32)
    values = jnp.where(kept_mask, jnp.exp((level_draw - 1.0) * weight_span), 0.0)
    diagonal = jax.random.uniform(diagonal_key, (block_count, TILE), dtype=jnp.float32, minval=0.5, maxval=1.0)
    unit_matrix = jnp.eye(TILE, dtype=jnp.float32)
    first_slot = values[:, 0] * (1.0 - unit_matrix)[None] + diagonal[:, :, None] * unit_matrix[None]
    values = jnp.concatenate([first_slot[:, None], values[:, 1:]], axis=1)
    return values.astype(jnp.bfloat16)


def draw_tiles_first(key, part):
    return tile_draw(jax.random.fold_in(key, 11), NODES_A // TILE)


def draw_tiles_second(key, part):
    return tile_draw(jax.random.fold_in(key, 13), NODES_B // TILE)


def draw_prior_scores(key, part):
    first_key, second_key = jax.random.split(jax.random.fold_in(key, 19))
    level_draw = jax.random.uniform(first_key, (NODES_A, NODES_B), dtype=jnp.float32)
    return jnp.exp((4.0 * level_draw - 3.0) * log_ten)


def draw_columns_first(key, part):
    block_count = NODES_A // TILE
    key_list = jax.random.split(key, block_count)
    return jax.vmap(lambda single: jax.random.permutation(single, block_count)[:SLOTS])(key_list).astype(jnp.int32)


def draw_columns_second(key, part):
    block_count = NODES_B // TILE
    key_list = jax.random.split(jax.random.fold_in(key, 7), block_count)
    return jax.vmap(lambda single: jax.random.permutation(single, block_count)[:SLOTS])(key_list).astype(jnp.int32)


def setup_inputs(seed: int = 0) -> dict:
    streams_of = jax.random.split(jax.random.key(seed), 6)
    return {
        "prior_scores": draw_prior_scores(jax.random.fold_in(streams_of[5], 71), 0),
        "tiles_first": draw_tiles_first(jax.random.fold_in(streams_of[5], 71), 0),
        "columns_first": draw_columns_first(jax.random.fold_in(streams_of[5], 71), 0),
        "tiles_second": draw_tiles_second(jax.random.fold_in(streams_of[5], 71), 0),
        "columns_second": draw_columns_second(jax.random.fold_in(streams_of[5], 71), 0),
    }


mixing = 0.8


def second_product(current, tile_set, columns, inverse):
    node_count = current.shape[0]
    blocks = current.reshape(node_count, -1, TILE)

    def per_block(operands):
        tiles_here, columns_here = operands
        picked = jnp.take(blocks, columns_here.astype(jnp.int32), axis=1).reshape(node_count, SLOTS * TILE)
        weight = tiles_here.transpose(0, 2, 1).reshape(SLOTS * TILE, TILE)
        return jnp.dot(picked, weight, preferred_element_type=jnp.float32)

    result = lax.map(per_block, (tile_set, columns))
    result = result.transpose(1, 0, 2).reshape(node_count, -1) * inverse[None, :]
    return result.astype(jnp.bfloat16)


def first_product(mixed_rows, tile_set, columns, inverse):
    width_b = mixed_rows.shape[1]
    blocks = mixed_rows.reshape(-1, TILE, width_b)

    def per_block(operands):
        tiles_here, columns_here = operands
        picked = jnp.take(blocks, columns_here.astype(jnp.int32), axis=0).reshape(SLOTS * TILE, width_b)
        weight = tiles_here.transpose(1, 0, 2).reshape(TILE, SLOTS * TILE)
        return jnp.dot(weight, picked, preferred_element_type=jnp.float32)

    result = lax.map(per_block, (tile_set, columns))
    result = result.reshape(-1, width_b) * inverse[:, None]
    return result.astype(jnp.bfloat16)


def reference(prior_scores, tiles_first, columns_first, tiles_second, columns_second):
    inverse_first = 1.0 / jnp.sum(tiles_first, axis=(1, 3), dtype=jnp.float32).reshape(-1)
    inverse_second = 1.0 / jnp.sum(tiles_second, axis=(1, 3), dtype=jnp.float32).reshape(-1)
    current_state = prior_scores
    for iteration in range(ITERS):
        current = current_state.astype(jnp.bfloat16)
        mixed_rows = second_product(current, tiles_second, columns_second, inverse_second)
        propagated = first_product(mixed_rows, tiles_first, columns_first, inverse_first)
        updated = mixing * propagated.astype(jnp.float32) + (1.0 - mixing) * prior_scores
        current_state = updated / (jnp.sum(updated) / float(NODES_A * NODES_B))
    return current_state
```

```python
import functools

import jax
import jax.numpy as jnp
from jax import lax
from jax.experimental import pallas as pl
from jax.experimental.pallas import tpu as pltpu
from jax.sharding import PartitionSpec as P

MESH = pl.DeviceIdType.MESH
BF = jnp.bfloat16
F32 = jnp.float32
MIX = 0.8
CELLS = float(12288 * 12288)
NT = (((1,), (1,)), ((), ()))
NN = (((1,), (0,)), ((), ()))


def half_lanes(shape):
    return lax.broadcasted_iota(jnp.int32, shape, 1) < 64


def swap(value):
    return pltpu.roll(value, 64, 1)


def main_kernel(
    prior, t1, t2, c1, c2,
    outf, outp, mout,
    prior_r, a1, a2, xr, zc, zpk, zsend, zspk, pfull, ppk, ph, prf, prp,
    mbuf, mpart, mtot, macc, c1g, c2g, c1s, c2s,
    lsem, ps_sem, pr_sem, cs_sem, cr_sem, ds_sem, dr_sem,
    gs_sem, gr_sem, xs_sem, xf_sem,
    zs_sem, zr_sem, fs_sem, ff_sem,
    qs_sem, qr_sem, os_sem, or_sem, ms_sem, mr_sem, mts_sem, mtr_sem,
):
    row = lax.axis_index("row")
    y = lax.axis_index("col")
    k = row % 2
    s = row // 2
    x = s % 4
    z = s // 4
    me = s * 4 + y

    def dev(s_, y_, k_):
        return {"row": s_ * 2 + k_, "col": y_}

    def remote(src, dst, ssem, rsem, target):
        return pltpu.make_async_remote_copy(
            src_ref=src, dst_ref=dst, send_sem=ssem, recv_sem=rsem,
            device_id=target, device_id_type=MESH,
        )

    barrier = pltpu.get_barrier_semaphore()

    def greet(i, _):
        other = (row * 4 + y + i) % 128
        pl.semaphore_signal(
            barrier, inc=1, device_id={"row": other // 4, "col": other % 4}, device_id_type=MESH
        )
        return 0

    load1 = pltpu.make_async_copy(t1, a1.at[pl.ds(s * 1920, 1920)], lsem.at[0])
    load1.start()
    load2 = pltpu.make_async_copy(t2.at[pl.ds(k * 7680, 7680)], a2.at[0], lsem.at[1])
    load2.start()
    load3 = pltpu.make_async_copy(
        prior.at[:, pl.ds(pl.multiple_of(y * 32, 32), 32), :], prior_r.at[y], lsem.at[2]
    )
    load3.start()
    lax.fori_loop(1, 128, greet, 0)
    c1g[s] = c1[...]
    c2g[y] = c2[...]
    xr[:, 192:208, :] = jnp.ones((96, 16, 128), BF)
    pl.semaphore_wait(barrier, 127)

    slice_copies, prior_copies, col_copies = [], [], []
    for d in (1, 3, 2):
        yd = (y + d) % 4
        cp = remote(
            t2.at[pl.ds(k * 7680 + s * 480, 480)],
            a2.at[(4 - d) % 4, pl.ds(s * 480, 480)],
            ds_sem.at[d], dr_sem.at[d], dev(s, yd, k),
        )
        cp.start()
        slice_copies.append(cp)
        cc = remote(c2, c2g.at[y], cs_sem.at[16 + d], cr_sem.at[16 + d], dev(s, yd, k))
        cc.start()
        col_copies.append(cc)

    XP, XM = (z * 4 + (x + 1) % 4), (z * 4 + (x + 3) % 4)
    ZP, ZM = (((z + 1) % 4) * 4 + x), (((z + 3) % 4) * 4 + x)

    def region(kind, origin, part):
        if kind == 0:
            off, size = ((0, 480), (480, 480), (960, 480), (1440, 480), (0, 960), (960, 960))[part]
            return a1.at[pl.ds(pl.multiple_of(origin * 1920 + off, 16), size)]
        off, size = ((0, 128), (128, 112), (240, 128), (368, 112), (0, 240), (240, 240))[part]
        return a2.at[pl.ds(1, 3), pl.ds(pl.multiple_of(origin * 480 + off, 16), size)]

    def nbr(axis, up):
        return (XP if up else XM) if axis == 0 else (ZP if up else ZM)

    def shifted(axis, origin, delta):
        ox, oz = origin % 4, origin // 4
        if axis == 0:
            return oz * 4 + (ox + delta) % 4
        return ((oz + delta) % 4) * 4 + ox

    gather_copies = []

    def hop(kind, half, group, slot, origin, part, axis, up):
        cp = remote(
            region(kind, origin, part), region(kind, origin, part),
            gs_sem.at[kind, half, group, slot], gr_sem.at[kind, half, group, slot],
            dev(nbr(axis, up), y, k),
        )
        cp.start()
        gather_copies.append(cp)

    def landed(kind, half, group, slot, origin, part):
        cp = remote(
            region(kind, origin, part), region(kind, origin, part),
            gs_sem.at[kind, half, group, slot], gr_sem.at[kind, half, group, slot],
            dev(nbr(0, True), y, k),
        )
        cp.wait_recv()

    def whole(half):
        return 4 + half

    def ring_start(kind, half, group, origin, axis):
        hop(kind, half, group, 0, origin, whole(half), axis, True)
        hop(kind, half, group, 1, origin, whole(half), axis, False)

    def ring_relay(kind, half, group, base, axis):
        low, high = shifted(axis, base, 3), shifted(axis, base, 1)
        landed(kind, half, group, 0, low, whole(half))
        hop(kind, half, group, 2, low, 2 * half, axis, True)
        landed(kind, half, group, 1, high, whole(half))
        hop(kind, half, group, 3, high, 2 * half + 1, axis, False)

    def ring_end(kind, half, group, base, axis):
        far = shifted(axis, base, 2)
        landed(kind, half, group, 2, far, 2 * half)
        landed(kind, half, group, 3, far, 2 * half + 1)

    def stage1(kind):
        for half in (0, 1):
            ring_start(kind, half, 0, s, half)
        for half in (0, 1):
            ring_start(kind, half, 1, s, 1 - half)

    def stage2(kind):
        for half in (0, 1):
            ring_relay(kind, half, 0, s, half)
            for g, delta in ((2, 3), (3, 1)):
                ring_start(kind, half, g, shifted(half, s, delta), 1 - half)

    def stage3(kind):
        for half in (0, 1):
            ring_end(kind, half, 0, s, half)
            ring_start(kind, half, 4, shifted(half, s, 2), 1 - half)

    def stage4(kind):
        for g, delta in ((1, 0), (2, 3), (3, 1), (4, 2)):
            for half in (0, 1):
                ring_relay(kind, half, g, shifted(half, s, delta), 1 - half)

    def stage5(kind):
        for g, delta in ((1, 0), (2, 3), (3, 1), (4, 2)):
            for half in (0, 1):
                ring_end(kind, half, g, shifted(half, s, delta), 1 - half)

    load1.wait()
    stage1(0)
    for d in (1, 3, 2):
        yd = (y + d) % 4
        cp = remote(
            prior.at[:, pl.ds(pl.multiple_of(yd * 32, 32), 32), :], prior_r.at[y],
            ps_sem.at[d], pr_sem.at[d], dev(s, yd, k),
        )
        cp.start()
        prior_copies.append(cp)

    def send_columns(i, _):
        remote(
            c1, c1g.at[s], cs_sem.at[i], cr_sem.at[i], dev((s + i) % 16, y, k)
        ).start()
        return 0

    lax.fori_loop(1, 16, send_columns, 0)

    for cp in slice_copies:
        cp.wait()
    stage1(1)
    stage2(0)
    stage2(1)
    stage3(0)
    stage3(1)
    load3.wait()
    load2.wait()

    for cc in col_copies:
        cc.wait()

    def wait_columns(i, _):
        remote(
            c1, c1g.at[(s + 16 - i) % 16], cs_sem.at[i], cr_sem.at[i], dev((s + i) % 16, y, k)
        ).wait()
        return 0

    lax.fori_loop(1, 16, wait_columns, 0)
    cps = [
        pltpu.make_async_copy(c1g, c1s, lsem.at[3]),
        pltpu.make_async_copy(c2g, c2s, lsem.at[4]),
    ]
    for cp in cps:
        cp.start()
    for cp in cps:
        cp.wait()

    stage4(1)
    stage4(0)
    for cp in prior_copies:
        cp.wait()

    mask96 = half_lanes((96, 128))
    mask48 = half_lanes((48, 128))

    def forward_state(group):
        return remote(
            xr.at[pl.ds(group * 3, 3), pl.ds(k * 96, 96)],
            xr.at[pl.ds(group * 3, 3), pl.ds(k * 96, 96)],
            xs_sem.at[group], xf_sem.at[group], dev(s, y, 1 - k),
        )

    def state_wait(group):
        remote(
            xr.at[pl.ds(group * 3, 3), pl.ds((1 - k) * 96, 96)],
            xr.at[pl.ds(group * 3, 3), pl.ds((1 - k) * 96, 96)],
            xs_sem.at[group], xf_sem.at[group], dev(s, y, 1 - k),
        ).wait()

    macc[...] = jnp.zeros((8, 128), F32)

    def convert(group, _):
        ys = group // 8
        for t in range(3):
            col = pl.multiple_of((group % 8) * 384 + t * 128, 128)
            value = prior_r[ys, :, :, pl.ds(col, 128)].reshape(96, 128)
            macc[...] += jnp.sum(value.reshape(12, 8, 128), axis=0)
            xr[group * 3 + t, pl.ds(pl.multiple_of(k * 96, 16), 96), :] = value.astype(BF)

        @pl.when(group > 0)
        def _():
            forward_state(group - 1).start()

        return 0

    lax.fori_loop(0, 32, convert, 0)
    forward_state(31).start()
    stage5(1)

    def state_done(group, _):
        state_wait(group)
        return 0

    def z_places(src_s, src_y, p):
        return (
            (
                pl.ds((src_s * 2 + p) * 3, 3),
                pl.ds(pl.multiple_of(src_y * 32, 32), 32),
                pl.ds(0, 128),
            ),
            (
                pl.ds(src_s * 3, 3),
                pl.ds(pl.multiple_of(src_y * 32 + p * 16, 16), 16),
                pl.ds(0, 128),
            ),
        )

    def z_copies(i, fn):
        yd = (y + i // 4) % 4
        g = (i + s) % 4
        for d in range(2):
            sd = k * 8 + g * 2 + d
            slot = yd * 8 + g * 2 + d
            for p in range(2):
                self_part = jnp.logical_and(jnp.logical_and(sd == s, yd == y), k == p)
                full_at, packed_at = z_places(s, y, p)
                full = remote(
                    zsend.at[slot, p], zc.at[full_at],
                    zs_sem.at[slot, p, 0], zr_sem.at[me, 0], dev(sd, yd, p),
                )
                packed = remote(
                    zspk.at[slot, :, pl.ds(p * 16, 16), :], zpk.at[packed_at],
                    zs_sem.at[slot, p, 1], zr_sem.at[me, 1], dev(sd, yd, p),
                )

                @pl.when(jnp.logical_not(self_part))
                def _():
                    fn(full)
                    fn(packed)

                if fn is begin:

                    @pl.when(self_part)
                    def _():
                        zc[full_at] = zsend[slot, p]
                        zpk[packed_at] = zspk[slot, :, p * 16 : p * 16 + 16, :]

    def begin(cp):
        cp.start()

    def end_send(cp):
        cp.wait_send()

    def z_compute(i, _):
        yd = (y + i // 4) % 4
        g = (i + s) % 4
        yr = i // 4
        values = []
        for t in range(3):
            jl = g * 3 + t
            acc = None
            for slot in range(5):
                c = c2s[yd, k * 12 + jl, slot]
                tile = a2[yr, pl.ds(pl.multiple_of((jl * 5 + slot) * 128, 128), 128), :]
                part = lax.dot_general(xr[c], tile, NT, preferred_element_type=F32)
                acc = part if acc is None else acc + part
            inv = 1.0 / acc[192:193, :]
            values.append(acc[0:192, :] * inv)
        out = yd * 8 + g * 2
        for p in range(2):
            rows = slice(p * 96, p * 96 + 96)
            zsend[out, p] = values[0][rows].astype(BF).reshape(3, 32, 128)
            zsend[out + 1, p] = values[2][rows].astype(BF).reshape(3, 32, 128)
        top, bottom = values[1][0:96], values[1][96:192]
        even = jnp.where(mask96, top, swap(bottom))
        odd = jnp.where(mask96, swap(top), bottom)
        zspk[out] = even.astype(BF).reshape(3, 32, 128)
        zspk[out + 1] = odd.astype(BF).reshape(3, 32, 128)

        @pl.when(i > 0)
        def _():
            z_copies(i - 1, begin)

        return 0

    def z_forward(src_s, src_y):
        src = src_s * 4 + src_y
        full_at, packed_at = z_places(src_s, src_y, k)
        full = remote(
            zc.at[full_at], zc.at[full_at],
            fs_sem.at[src, 0], ff_sem.at[src, 0], dev(s, y, 1 - k),
        )
        packed = remote(
            zpk.at[packed_at], zpk.at[packed_at],
            fs_sem.at[src, 1], ff_sem.at[src, 1], dev(s, y, 1 - k),
        )
        return full, packed

    def z_receive(i, _):
        src_s = (s + i // 4) % 16
        src_y = (y + i) % 4
        src = src_s * 4 + src_y
        full, packed = z_forward(src_s, src_y)
        own = jnp.logical_and(src == me, s // 8 == k)

        @pl.when(jnp.logical_not(own))
        def _():
            full_at, packed_at = z_places(src_s, src_y, k)
            remote(
                zc.at[full_at], zc.at[full_at],
                fs_sem.at[src, 0], zr_sem.at[src, 0], dev(s, y, 1 - k),
            ).wait_recv()
            remote(
                zpk.at[packed_at], zpk.at[packed_at],
                fs_sem.at[src, 1], zr_sem.at[src, 1], dev(s, y, 1 - k),
            ).wait_recv()

        full.start()
        packed.start()
        return 0

    def z_finish(i, _):
        src_s = (s + i // 4) % 16
        src_y = (y + i) % 4
        src = src_s * 4 + src_y
        full_at, packed_at = z_places(src_s, src_y, 1 - k)
        remote(
            zc.at[full_at], zc.at[full_at],
            fs_sem.at[src, 0], ff_sem.at[src, 0], dev(s, y, 1 - k),
        ).wait()
        remote(
            zpk.at[packed_at], zpk.at[packed_at],
            fs_sem.at[src, 1], ff_sem.at[src, 1], dev(s, y, 1 - k),
        ).wait()
        return 0

    def z_unpack(i, _):
        packed = zpk[i].astype(F32)
        lane = lax.broadcasted_iota(jnp.int32, (128, 128), 1)
        fill = jnp.where(lane == 64, 1.0, 0.0).astype(F32)
        block = (i // 3) * 6 + i % 3
        zc[block, :, 128:256] = jnp.where(lane < 64, packed, fill).astype(BF)
        zc[block + 3, :, 128:256] = jnp.where(lane < 64, swap(packed), fill).astype(BF)
        return 0

    def second_stage():
        lax.fori_loop(0, 32, state_done, 0)
        lax.fori_loop(0, 16, z_compute, 0)
        z_copies(15, begin)
        lax.fori_loop(0, 64, z_receive, 0)
        lax.fori_loop(0, 64, z_finish, 0)

        def sent(i, _):
            z_copies(i, end_send)
            return 0

        lax.fori_loop(0, 16, sent, 0)
        lax.fori_loop(0, 48, z_unpack, 0)

    def p_copies(i, last, fn):
        sd = (s + i) % 16
        if last:
            full = (pfull.at[pl.ds(sd * 3, 3)], outf.at[s])
            packed = (ppk.at[sd], outp.at[s])
            pair = [
                remote(*full, os_sem.at[sd, 0], or_sem.at[s, 0], dev(sd, y, k)),
                remote(*packed, os_sem.at[sd, 1], or_sem.at[s, 1], dev(sd, y, k)),
            ]
            mine = [
                pltpu.make_async_copy(*full, lsem.at[5]),
                pltpu.make_async_copy(*packed, lsem.at[6]),
            ]

            @pl.when(sd != s)
            def _():
                for cp in pair:
                    fn(cp)

            @pl.when(sd == s)
            def _():
                for cp in mine:
                    if fn is begin:
                        cp.start()
                    else:
                        cp.wait()

            return
        for yd in range(4):
            own = jnp.logical_and(sd == s, y == yd)
            pair = [
                remote(
                    pfull.at[pl.ds(sd * 3, 3), pl.ds(yd * 32, 32)], prf.at[me],
                    qs_sem.at[sd * 4 + yd, 0], qr_sem.at[me, 0], dev(sd, yd, k),
                ),
                remote(
                    ppk.at[sd, yd], prp.at[me],
                    qs_sem.at[sd * 4 + yd, 1], qr_sem.at[me, 1], dev(sd, yd, k),
                ),
            ]

            @pl.when(jnp.logical_not(own))
            def _():
                for cp in pair:
                    fn(cp)

            if fn is begin:

                @pl.when(own)
                def _():
                    prf[me] = pfull[pl.ds(sd * 3, 3), pl.ds(yd * 32, 32), :]
                    prp[me] = ppk[sd, yd]

    def p_compute(last, i, _):
        sd = (s + i) % 16
        for t in range(3):
            acc = None
            for slot in range(5):
                c = c1s[sd, t, slot]
                tile = a1[pl.ds(pl.multiple_of((sd * 15 + t * 5 + slot) * 128, 128), 128), :]
                part = lax.dot_general(
                    tile, zc[c], NN, preferred_element_type=F32
                )
                acc = part if acc is None else acc + part
            inv = 1.0 / acc[:, 192:193]
            first = (acc[:, 0:128] * inv).astype(BF)
            second = (acc[:, 128:256] * inv).astype(BF).astype(F32)
            second = jnp.where(half_lanes((128, 128)), second, 0.0)
            total = first.astype(F32) + second
            mpart[...] += jnp.sum(total.reshape(16, 8, 128), axis=0)
            pfull[sd * 3 + t] = first
            ph[t] = second
        for yd in range(4):
            if last:
                flat = ph[...].reshape(384, 128)
                low = flat[yd * 48 : yd * 48 + 48]
                high = flat[192 + yd * 48 : 240 + yd * 48]
            else:
                low = ph[:, yd * 32 : yd * 32 + 16, :].reshape(48, 128)
                high = ph[:, yd * 32 + 16 : yd * 32 + 32, :].reshape(48, 128)
            ppk[sd, yd] = (low + swap(high)).astype(BF)

        @pl.when(i > 0)
        def _():
            p_copies(i - 1, last, begin)

        return 0

    def first_stage(last, it):
        mpart[...] = jnp.zeros((8, 128), F32)
        lax.fori_loop(0, 16, functools.partial(p_compute, last), 0)
        p_copies(15, last, begin)
        mbuf[it, me] = MIX * mpart[...] + (1.0 - MIX) * macc[...]
        mpart[...] = mbuf[it, me]

        def total_copy(i, src, dst):
            other = (me + i) % 64
            return remote(
                mpart, mbuf.at[it, src], ms_sem.at[i], mr_sem.at[i], dev(dst // 4, dst % 4, k)
            )

        def total_send(i, _):
            total_copy(i, me, (me + i) % 64).start()
            return 0

        def total_wait(i, _):
            total_copy(i, (me + 64 - i) % 64, (me + i) % 64).wait()
            return 0

        lax.fori_loop(1, 64, total_send, 0)
        lax.fori_loop(1, 64, total_wait, 0)
        mtot[it, 0] = jnp.sum(mbuf[it], axis=0)
        exchange = remote(
            mtot.at[it, 0], mtot.at[it, 1], mts_sem.at[it], mtr_sem.at[it], dev(s, y, 1 - k)
        )
        exchange.start()
        exchange.wait()
        grand = jnp.sum(mtot[it, 0] + mtot[it, 1])
        return jnp.full((8, 128), grand / CELLS, F32)

    def p_wait(src):
        src_dev = dev(src // 4, src % 4, k)

        @pl.when(src != me)
        def _():
            remote(
                prf.at[src], prf.at[src], qs_sem.at[src, 0], qr_sem.at[src, 0], src_dev
            ).wait_recv()
            remote(
                prp.at[src], prp.at[src], qs_sem.at[src, 1], qr_sem.at[src, 1], src_dev
            ).wait_recv()

    def update(scale, group, _):
        ys = group // 8
        even = ((group % 8) * 2) * 4 + ys
        odd = even + 4
        p_wait(even)
        p_wait(odd)
        a, b = prp[even].astype(F32), prp[odd].astype(F32)
        mid_top = jnp.where(mask48, a, swap(b))
        mid_bottom = jnp.where(mask48, swap(a), b)
        mid = jnp.concatenate(
            [mid_top.reshape(3, 16, 128), mid_bottom.reshape(3, 16, 128)], axis=1
        ).reshape(96, 128)
        first, third = prf[even].astype(F32), prf[odd].astype(F32)
        for t, value in enumerate((first.reshape(96, 128), mid, third.reshape(96, 128))):
            col = pl.multiple_of((group % 8) * 384 + t * 128, 128)
            before = prior_r[ys, :, :, pl.ds(col, 128)].reshape(96, 128)
            now = (MIX * value + (1.0 - MIX) * before) / scale
            xr[group * 3 + t, pl.ds(pl.multiple_of(k * 96, 16), 96), :] = now.astype(BF)

        @pl.when(group > 0)
        def _():
            forward_state(group - 1).start()

        return 0

    second_stage()
    stage5(0)
    for cp in gather_copies:
        cp.wait_send()
    m1 = first_stage(False, 0)
    scale = m1[0:1, :]
    lax.fori_loop(0, 32, functools.partial(update, scale), 0)
    forward_state(31).start()

    def p_sent(i, _):
        p_copies(i, False, end_send)
        return 0

    lax.fori_loop(0, 16, p_sent, 0)

    second_stage()
    mout[...] = first_stage(True, 1)

    def p_last(i, _):
        p_copies(i, True, end_send)
        return 0

    lax.fori_loop(0, 16, p_last, 0)

    def out_wait(i, _):
        src = (s + i) % 16
        remote(
            outf.at[src], outf.at[src], os_sem.at[src, 0], or_sem.at[src, 0], dev(src, y, k)
        ).wait_recv()
        remote(
            outp.at[src], outp.at[src], os_sem.at[src, 1], or_sem.at[src, 1], dev(src, y, k)
        ).wait_recv()
        return 0

    lax.fori_loop(1, 16, out_wait, 0)


def run_main(prior, t1, t2, c1, c2):
    any_spec = pl.BlockSpec(memory_space=pl.ANY)
    vmem = pl.BlockSpec(memory_space=pltpu.VMEM)
    dma = pltpu.SemaphoreType.DMA
    scratch = [
        pltpu.VMEM((4, 3, 32, 3072), F32),
        pltpu.VMEM((30720, 128), BF),
        pltpu.VMEM((4, 7680, 128), BF),
        pltpu.VMEM((96, 208, 128), BF),
        pltpu.VMEM((96, 128, 256), BF),
        pltpu.VMEM((48, 128, 128), BF),
        pltpu.VMEM((32, 2, 3, 32, 128), BF),
        pltpu.VMEM((32, 3, 32, 128), BF),
        pltpu.VMEM((48, 128, 128), BF),
        pltpu.VMEM((16, 4, 48, 128), BF),
        pltpu.VMEM((3, 128, 128), F32),
        pltpu.VMEM((64, 3, 32, 128), BF),
        pltpu.VMEM((64, 48, 128), BF),
        pltpu.VMEM((2, 64, 8, 128), F32),
        pltpu.VMEM((8, 128), F32),
        pltpu.VMEM((2, 2, 8, 128), F32),
        pltpu.VMEM((8, 128), F32),
        pltpu.VMEM((16, 8, 128), jnp.int32),
        pltpu.VMEM((4, 24, 128), jnp.int32),
        pltpu.SMEM((16, 8, 128), jnp.int32),
        pltpu.SMEM((4, 24, 128), jnp.int32),
        dma((7,)), dma((4,)), dma((4,)), dma((20,)), dma((20,)), dma((4,)), dma((4,)),
        dma((2, 2, 5, 4)), dma((2, 2, 5, 4)), dma((32,)), dma((32,)),
        dma((32, 2, 2)), dma((64, 2)), dma((64, 2)), dma((64, 2)),
        dma((64, 2)), dma((64, 2)), dma((16, 2)), dma((16, 2)),
        dma((64,)), dma((64,)), dma((2,)), dma((2,)),
    ]
    return pl.pallas_call(
        main_kernel,
        out_shape=(
            jax.ShapeDtypeStruct((16, 3, 128, 128), BF),
            jax.ShapeDtypeStruct((16, 4, 48, 128), BF),
            jax.ShapeDtypeStruct((8, 128), F32),
        ),
        in_specs=[any_spec, any_spec, any_spec, vmem, vmem],
        out_specs=(any_spec, any_spec, vmem),
        scratch_shapes=scratch,
        compiler_params=pltpu.CompilerParams(
            collective_id=0, has_side_effects=True, vmem_limit_bytes=60 << 20
        ),
        name="align",
    )(prior, t1, t2, c1, c2)


def combine_kernel(pf, pp, m, prior, out):
    mask = half_lanes((192, 128))
    scale = m[0:1, :]
    a, b = pp[0].astype(F32), pp[1].astype(F32)
    mid = jnp.concatenate([jnp.where(mask, a, swap(b)), jnp.where(mask, swap(a), b)], axis=0)
    for t, value in enumerate((pf[0].astype(F32), mid, pf[1].astype(F32))):
        cols = slice(t * 128, (t + 1) * 128)
        out[:, cols] = (MIX * value + (1.0 - MIX) * prior[:, cols]) / scale


def combine(pf, pp, m, prior):
    return pl.pallas_call(
        combine_kernel,
        grid=(8,),
        out_shape=jax.ShapeDtypeStruct((384, 3072), F32),
        in_specs=[
            pl.BlockSpec((2, 384, 128), lambda i: (i, 0, 0)),
            pl.BlockSpec((2, 192, 128), lambda i: (i, 0, 0)),
            pl.BlockSpec((8, 128), lambda i: (0, 0)),
            pl.BlockSpec((384, 384), lambda i: (0, i)),
        ],
        out_specs=pl.BlockSpec((384, 384), lambda i: (0, i)),
        name="combine",
    )(pf, pp, m, prior)


def local(prior_scores, tiles_first, columns_first, tiles_second, columns_second):
    t1 = tiles_first.reshape(1920, 128)
    t2 = tiles_second.reshape(15360, 128)
    c1 = jnp.pad(columns_first.astype(jnp.int32), ((0, 5), (0, 123)))
    c2 = jnp.pad(columns_second.astype(jnp.int32), ((0, 0), (0, 123)))
    pf, pp, m = run_main(prior_scores.reshape(3, 128, 3072), t1, t2, c1, c2)
    return combine(
        pf.reshape(16, 384, 128), pp.reshape(16, 192, 128), m, prior_scores
    )


def solution(mesh):
    return jax.shard_map(
        local,
        mesh=mesh,
        in_specs=(
            P("row", "col"),
            P("row", None, None, None),
            P("row", None),
            P("col", None, None, None),
            P("col", None),
        ),
        out_specs=P("row", "col"),
        check_vma=False,
    )
```

```python
import functools

import jax
import jax.numpy as jnp
from jax import lax
from jax.experimental import pallas as pl
from jax.experimental.pallas import tpu as pltpu
from jax.sharding import PartitionSpec as P

MESH = pl.DeviceIdType.MESH
BF = jnp.bfloat16
F32 = jnp.float32
MIX = 0.8
CELLS = float(12288 * 12288)
HELD = 8
NT = (((1,), (1,)), ((), ()))
NN = (((1,), (0,)), ((), ()))


def half_lanes(shape):
    return lax.broadcasted_iota(jnp.int32, shape, 1) < 64


def swap(value):
    return pltpu.roll(value, 64, 1)


def main_kernel(
    prior, t1, t2, c1, c2,
    outf, outp, mout,
    prior_r, a1, a2, xr, zc, zpk, zsend, zspk, pfull, ppk, ph, prf, prp,
    mbuf, msend, mpart, mtot, macc, c1g, c2g, c1s, c2s,
    lsem, ps_sem, pr_sem, cs_sem, cr_sem, ds_sem, dr_sem,
    gs_sem, gr_sem, xs_sem, xf_sem,
    zs_sem, zr_sem, fs_sem, ff_sem,
    qs_sem, qr_sem, os_sem, or_sem, ms_sem, mr_sem, mts_sem, mtr_sem,
):
    row = lax.axis_index("row")
    y = lax.axis_index("col")
    k = row % 2
    s = row // 2
    x = s % 4
    z = s // 4
    me = s * 4 + y

    def dev(s_, y_, k_):
        return {"row": s_ * 2 + k_, "col": y_}

    def remote(src, dst, ssem, rsem, target):
        return pltpu.make_async_remote_copy(
            src_ref=src, dst_ref=dst, send_sem=ssem, recv_sem=rsem,
            device_id=target, device_id_type=MESH,
        )

    barrier = pltpu.get_barrier_semaphore()

    def greet(i, _):
        other = (row * 4 + y + i) % 128
        pl.semaphore_signal(
            barrier, inc=1, device_id={"row": other // 4, "col": other % 4}, device_id_type=MESH
        )
        return 0

    load1 = pltpu.make_async_copy(t1, a1.at[pl.ds(s * 1920, 1920)], lsem.at[0])
    load1.start()
    load2 = pltpu.make_async_copy(t2.at[pl.ds(k * 7680, 7680)], a2.at[0], lsem.at[1])
    load2.start()
    load3 = pltpu.make_async_copy(
        prior.at[:, pl.ds(pl.multiple_of(y * 32, 32), 32), :], prior_r.at[y], lsem.at[2]
    )
    load3.start()
    lax.fori_loop(1, 128, greet, 0)
    c1g[s] = c1[...]
    c2g[y] = c2[...]
    xr[:, 192:208, :] = jnp.ones((96, 16, 128), BF)
    pl.semaphore_wait(barrier, 127)

    slice_copies, prior_copies, col_copies = [], [], []
    for d in (1, 3, 2):
        yd = (y + d) % 4
        cp = remote(
            t2.at[pl.ds(k * 7680 + s * 480, 480)],
            a2.at[(4 - d) % 4, pl.ds(s * 480, 480)],
            ds_sem.at[d], dr_sem.at[d], dev(s, yd, k),
        )
        cp.start()
        slice_copies.append(cp)
        cc = remote(c2, c2g.at[y], cs_sem.at[16 + d], cr_sem.at[16 + d], dev(s, yd, k))
        cc.start()
        col_copies.append(cc)

    XP, XM = (z * 4 + (x + 1) % 4), (z * 4 + (x + 3) % 4)
    ZP, ZM = (((z + 1) % 4) * 4 + x), (((z + 3) % 4) * 4 + x)

    def region(kind, origin, part):
        if kind == 0:
            off, size = ((0, 480), (480, 480), (960, 480), (1440, 480), (0, 960), (960, 960))[part]
            return a1.at[pl.ds(pl.multiple_of(origin * 1920 + off, 16), size)]
        off, size = ((0, 128), (128, 112), (240, 128), (368, 112), (0, 240), (240, 240))[part]
        return a2.at[pl.ds(1, 3), pl.ds(pl.multiple_of(origin * 480 + off, 16), size)]

    def nbr(axis, up):
        return (XP if up else XM) if axis == 0 else (ZP if up else ZM)

    def shifted(axis, origin, delta):
        ox, oz = origin % 4, origin // 4
        if axis == 0:
            return oz * 4 + (ox + delta) % 4
        return ((oz + delta) % 4) * 4 + ox

    gather_copies = []

    def hop(kind, half, group, slot, origin, part, axis, up):
        cp = remote(
            region(kind, origin, part), region(kind, origin, part),
            gs_sem.at[kind, half, group, slot], gr_sem.at[kind, half, group, slot],
            dev(nbr(axis, up), y, k),
        )
        cp.start()
        gather_copies.append(cp)

    def landed(kind, half, group, slot, origin, part):
        cp = remote(
            region(kind, origin, part), region(kind, origin, part),
            gs_sem.at[kind, half, group, slot], gr_sem.at[kind, half, group, slot],
            dev(nbr(0, True), y, k),
        )
        cp.wait_recv()

    def whole(half):
        return 4 + half

    def ring_start(kind, half, group, origin, axis):
        hop(kind, half, group, 0, origin, whole(half), axis, True)
        hop(kind, half, group, 1, origin, whole(half), axis, False)

    def ring_relay(kind, half, group, base, axis):
        low, high = shifted(axis, base, 3), shifted(axis, base, 1)
        landed(kind, half, group, 0, low, whole(half))
        hop(kind, half, group, 2, low, 2 * half, axis, True)
        landed(kind, half, group, 1, high, whole(half))
        hop(kind, half, group, 3, high, 2 * half + 1, axis, False)

    def ring_end(kind, half, group, base, axis):
        far = shifted(axis, base, 2)
        landed(kind, half, group, 2, far, 2 * half)
        landed(kind, half, group, 3, far, 2 * half + 1)

    def stage1(kind):
        for half in (0, 1):
            ring_start(kind, half, 0, s, half)
        for half in (0, 1):
            ring_start(kind, half, 1, s, 1 - half)

    def stage2(kind):
        for half in (0, 1):
            ring_relay(kind, half, 0, s, half)
            for g, delta in ((2, 3), (3, 1)):
                ring_start(kind, half, g, shifted(half, s, delta), 1 - half)

    def stage3(kind):
        for half in (0, 1):
            ring_end(kind, half, 0, s, half)
            ring_start(kind, half, 4, shifted(half, s, 2), 1 - half)

    def stage4(kind):
        for g, delta in ((1, 0), (2, 3), (3, 1), (4, 2)):
            for half in (0, 1):
                ring_relay(kind, half, g, shifted(half, s, delta), 1 - half)

    def stage5(kind):
        for g, delta in ((1, 0), (2, 3), (3, 1), (4, 2)):
            for half in (0, 1):
                ring_end(kind, half, g, shifted(half, s, delta), 1 - half)

    load1.wait()
    stage1(0)
    for d in (1, 3, 2):
        yd = (y + d) % 4
        cp = remote(
            prior.at[:, pl.ds(pl.multiple_of(yd * 32, 32), 32), :], prior_r.at[y],
            ps_sem.at[d], pr_sem.at[d], dev(s, yd, k),
        )
        cp.start()
        prior_copies.append(cp)

    def send_columns(i, _):
        remote(
            c1, c1g.at[s], cs_sem.at[i], cr_sem.at[i], dev((s + i) % 16, y, k)
        ).start()
        return 0

    lax.fori_loop(1, 16, send_columns, 0)

    for cp in slice_copies:
        cp.wait()
    stage1(1)
    stage2(0)
    stage2(1)
    stage3(0)
    stage3(1)
    load3.wait()
    load2.wait()

    for cc in col_copies:
        cc.wait()

    def wait_columns(i, _):
        remote(
            c1, c1g.at[(s + 16 - i) % 16], cs_sem.at[i], cr_sem.at[i], dev((s + i) % 16, y, k)
        ).wait()
        return 0

    lax.fori_loop(1, 16, wait_columns, 0)
    cps = [
        pltpu.make_async_copy(c1g, c1s, lsem.at[3]),
        pltpu.make_async_copy(c2g, c2s, lsem.at[4]),
    ]
    for cp in cps:
        cp.start()
    for cp in cps:
        cp.wait()

    stage4(1)
    stage4(0)
    for cp in prior_copies:
        cp.wait()

    mask96 = half_lanes((96, 128))
    mask48 = half_lanes((48, 128))

    def forward_state(group):
        return remote(
            xr.at[pl.ds(group * 3, 3), pl.ds(k * 96, 96)],
            xr.at[pl.ds(group * 3, 3), pl.ds(k * 96, 96)],
            xs_sem.at[group], xf_sem.at[group], dev(s, y, 1 - k),
        )

    def state_wait(group):
        remote(
            xr.at[pl.ds(group * 3, 3), pl.ds((1 - k) * 96, 96)],
            xr.at[pl.ds(group * 3, 3), pl.ds((1 - k) * 96, 96)],
            xs_sem.at[group], xf_sem.at[group], dev(s, y, 1 - k),
        ).wait()

    macc[...] = jnp.zeros((8, 128), F32)

    def convert(group, _):
        ys = group // 8
        for t in range(3):
            col = pl.multiple_of((group % 8) * 384 + t * 128, 128)
            value = prior_r[ys, :, :, pl.ds(col, 128)].reshape(96, 128)
            macc[...] += jnp.sum(value.reshape(12, 8, 128), axis=0)
            xr[group * 3 + t, pl.ds(pl.multiple_of(k * 96, 16), 96), :] = value.astype(BF)

        @pl.when(group > 0)
        def _():
            forward_state(group - 1).start()

        return 0

    lax.fori_loop(0, 32, convert, 0)
    forward_state(31).start()
    stage5(1)

    def state_done(group, _):
        state_wait(group)
        return 0

    def z_places(src_s, src_y, p):
        return (
            (
                pl.ds((src_s * 2 + p) * 3, 3),
                pl.ds(pl.multiple_of(src_y * 32, 32), 32),
                pl.ds(0, 128),
            ),
            (
                pl.ds(src_s * 3, 3),
                pl.ds(pl.multiple_of(src_y * 32 + p * 16, 16), 16),
                pl.ds(0, 128),
            ),
        )

    ZG = x + 2 * z

    def z_copies(i, fn):
        yd = (y + i) % 4
        g = (i // 4 + ZG) % 4
        for d in range(2):
            sd = k * 8 + g * 2 + d
            slot = yd * 8 + g * 2 + d
            for p in range(2):
                self_part = jnp.logical_and(jnp.logical_and(sd == s, yd == y), k == p)
                full_at, packed_at = z_places(s, y, p)
                full = remote(
                    zsend.at[slot, p], zc.at[full_at],
                    zs_sem.at[slot, p, 0], zr_sem.at[me, 0], dev(sd, yd, p),
                )
                packed = remote(
                    zspk.at[slot, :, pl.ds(p * 16, 16), :], zpk.at[packed_at],
                    zs_sem.at[slot, p, 1], zr_sem.at[me, 1], dev(sd, yd, p),
                )

                @pl.when(jnp.logical_not(self_part))
                def _():
                    fn(full)
                    fn(packed)

                if fn is begin:

                    @pl.when(self_part)
                    def _():
                        zc[full_at] = zsend[slot, p]
                        zpk[packed_at] = zspk[slot, :, p * 16 : p * 16 + 16, :]

    def begin(cp):
        cp.start()

    def end_send(cp):
        cp.wait_send()

    def z_compute(i, _):
        yd = (y + i) % 4
        g = (i // 4 + ZG) % 4
        yr = i % 4
        values = []
        for t in range(3):
            jl = g * 3 + t
            acc = None
            for slot in range(5):
                c = c2s[yd, k * 12 + jl, slot]
                tile = a2[yr, pl.ds(pl.multiple_of((jl * 5 + slot) * 128, 128), 128), :]
                part = lax.dot_general(xr[c], tile, NT, preferred_element_type=F32)
                acc = part if acc is None else acc + part
            inv = 1.0 / acc[192:193, :]
            values.append(acc[0:192, :] * inv)
        out = yd * 8 + g * 2
        for p in range(2):
            rows = slice(p * 96, p * 96 + 96)
            zsend[out, p] = values[0][rows].astype(BF).reshape(3, 32, 128)
            zsend[out + 1, p] = values[2][rows].astype(BF).reshape(3, 32, 128)
        top, bottom = values[1][0:96], values[1][96:192]
        even = jnp.where(mask96, top, swap(bottom))
        odd = jnp.where(mask96, swap(top), bottom)
        zspk[out] = even.astype(BF).reshape(3, 32, 128)
        zspk[out + 1] = odd.astype(BF).reshape(3, 32, 128)

        @pl.when(i > 0)
        def _():
            z_copies(i - 1, begin)

        return 0

    def z_forward(src_s, src_y):
        src = src_s * 4 + src_y
        full_at, packed_at = z_places(src_s, src_y, k)
        full = remote(
            zc.at[full_at], zc.at[full_at],
            fs_sem.at[src, 0], ff_sem.at[src, 0], dev(s, y, 1 - k),
        )
        packed = remote(
            zpk.at[packed_at], zpk.at[packed_at],
            fs_sem.at[src, 1], ff_sem.at[src, 1], dev(s, y, 1 - k),
        )
        return full, packed

    def z_source(n):
        c = ((s % 8) // 2 + 4 - n // 16) % 4
        r = (n // 4) % 4
        xs = c % 2 + 2 * (r % 2)
        zs = ((c + 4 - xs) // 2) % 2 + 2 * (r // 2)
        return zs * 4 + xs, (y + 4 - n % 4) % 4

    def z_receive(i, _):
        src_s, src_y = z_source(i)
        src = src_s * 4 + src_y
        full, packed = z_forward(src_s, src_y)
        own = jnp.logical_and(src == me, s // 8 == k)

        @pl.when(jnp.logical_not(own))
        def _():
            full_at, packed_at = z_places(src_s, src_y, k)
            remote(
                zc.at[full_at], zc.at[full_at],
                fs_sem.at[src, 0], zr_sem.at[src, 0], dev(s, y, 1 - k),
            ).wait_recv()
            remote(
                zpk.at[packed_at], zpk.at[packed_at],
                fs_sem.at[src, 1], zr_sem.at[src, 1], dev(s, y, 1 - k),
            ).wait_recv()

        full.start()
        packed.start()
        return 0

    def z_finish(i, _):
        src_s, src_y = z_source(i)
        src = src_s * 4 + src_y
        full_at, packed_at = z_places(src_s, src_y, 1 - k)
        remote(
            zc.at[full_at], zc.at[full_at],
            fs_sem.at[src, 0], ff_sem.at[src, 0], dev(s, y, 1 - k),
        ).wait()
        remote(
            zpk.at[packed_at], zpk.at[packed_at],
            fs_sem.at[src, 1], ff_sem.at[src, 1], dev(s, y, 1 - k),
        ).wait()
        return 0

    def z_unpack(n, _):
        i = z_source((n // 3) * 4)[0] * 3 + n % 3
        packed = zpk[i].astype(F32)
        lane = lax.broadcasted_iota(jnp.int32, (128, 128), 1)
        fill = jnp.where(lane == 64, 1.0, 0.0).astype(F32)
        block = (i // 3) * 6 + i % 3
        zc[block, :, 128:256] = jnp.where(lane < 64, packed, fill).astype(BF)
        zc[block + 3, :, 128:256] = jnp.where(lane < 64, swap(packed), fill).astype(BF)
        return 0

    def second_stage():
        lax.fori_loop(0, 32, state_done, 0)
        lax.fori_loop(0, 16, z_compute, 0)
        z_copies(15, begin)
        for phase in range(5):
            if phase < 4:
                lax.fori_loop(phase * 16, phase * 16 + 16, z_receive, 0)
            if phase > 0:
                lax.fori_loop(phase * 16 - 16, phase * 16, z_finish, 0)
                lax.fori_loop(phase * 12 - 12, phase * 12, z_unpack, 0)

        def sent(i, _):
            z_copies(i, end_send)
            return 0

        lax.fori_loop(0, 16, sent, 0)

    def partner_at(i, sign):
        j = i // 2
        dz = (j % 4) * (1 + 2 * k) * sign
        xa = (x + 2 * ((j // 4 + j) % 2)) % 4
        return ((z + dz) % 4) * 4 + xa + (i % 2) * (1 - 2 * (xa % 2))

    def target(i):
        return partner_at(i, 1)

    def p_copies(i, last, fn):
        sd = target(i)
        if last:
            full = (pfull.at[pl.ds(sd * 3, 3)], outf.at[s])
            packed = (ppk.at[sd], outp.at[s])
            pair = [
                remote(*full, os_sem.at[sd, 0], or_sem.at[s, 0], dev(sd, y, k)),
                remote(*packed, os_sem.at[sd, 1], or_sem.at[s, 1], dev(sd, y, k)),
            ]
            mine = [
                pltpu.make_async_copy(*full, lsem.at[5]),
                pltpu.make_async_copy(*packed, lsem.at[6]),
            ]

            @pl.when(sd != s)
            def _():
                for cp in pair:
                    fn(cp)

            @pl.when(sd == s)
            def _():
                for cp in mine:
                    if fn is begin:
                        cp.start()
                    else:
                        cp.wait()

            return
        for step in range(4):
            yd = (y + step) % 4
            pair = [
                remote(
                    pfull.at[pl.ds(sd * 3, 3), pl.ds(pl.multiple_of(yd * 32, 32), 32)], prf.at[me],
                    qs_sem.at[sd * 4 + yd, 0], qr_sem.at[me, 0], dev(sd, yd, k),
                ),
                remote(
                    ppk.at[sd, yd], prp.at[me],
                    qs_sem.at[sd * 4 + yd, 1], qr_sem.at[me, 1], dev(sd, yd, k),
                ),
            ]

            if step > 0:
                for cp in pair:
                    fn(cp)
                continue

            @pl.when(sd != s)
            def _():
                for cp in pair:
                    fn(cp)

            if fn is begin:

                @pl.when(sd == s)
                def _():
                    prf[me] = pfull[pl.ds(sd * 3, 3), pl.ds(pl.multiple_of(y * 32, 32), 32), :]
                    prp[me] = ppk[sd, y]

    def p_compute(last, i, _):
        sd = target(i)
        for t in range(3):
            acc = None
            for slot in range(5):
                c = c1s[sd, t, slot]
                tile = a1[pl.ds(pl.multiple_of((sd * 15 + t * 5 + slot) * 128, 128), 128), :]
                part = lax.dot_general(
                    tile, zc[c], NN, preferred_element_type=F32
                )
                acc = part if acc is None else acc + part
            inv = 1.0 / acc[:, 192:193]
            first = (acc[:, 0:128] * inv).astype(BF)
            second = (acc[:, 128:256] * inv).astype(BF).astype(F32)
            second = jnp.where(half_lanes((128, 128)), second, 0.0)
            total = first.astype(F32) + second
            mpart[...] += jnp.sum(total.reshape(16, 8, 128), axis=0)
            pfull[sd * 3 + t] = first
            ph[t] = second
        for yd in range(4):
            if last:
                flat = ph[...].reshape(384, 128)
                low = flat[yd * 48 : yd * 48 + 48]
                high = flat[192 + yd * 48 : 240 + yd * 48]
            else:
                low = ph[:, yd * 32 : yd * 32 + 16, :].reshape(48, 128)
                high = ph[:, yd * 32 + 16 : yd * 32 + 32, :].reshape(48, 128)
            ppk[sd, yd] = (low + swap(high)).astype(BF)

        @pl.when(jnp.logical_and(i > 0, i <= HELD))
        def _():
            p_copies(i - 1, last, begin)

        return 0

    def first_stage(last, it):
        mpart[...] = jnp.zeros((8, 128), F32)
        lax.fori_loop(0, 16, functools.partial(p_compute, last), 0)
        mine = jnp.sum(MIX * mpart[...] + (1.0 - MIX) * macc[...], axis=0, keepdims=True)
        mbuf[it, me] = mine
        msend[it] = mine

        def total_copy(i, src, dst):
            other = (me + i) % 64
            return remote(
                msend.at[it], mbuf.at[it, src], ms_sem.at[i], mr_sem.at[i], dev(dst // 4, dst % 4, k)
            )

        def total_send(i, _):
            total_copy(i, me, (me + i) % 64).start()
            return 0

        def total_wait(i, _):
            total_copy(i, (me + 64 - i) % 64, (me + i) % 64).wait()
            return 0

        def late(i, _):
            p_copies(i, last, begin)
            return 0

        lax.fori_loop(1, 64, total_send, 0)
        lax.fori_loop(HELD, 16, late, 0)
        lax.fori_loop(1, 64, total_wait, 0)
        mtot[it, 0] = jnp.sum(mbuf[it], axis=0)
        exchange = remote(
            mtot.at[it, 0], mtot.at[it, 1], mts_sem.at[it], mtr_sem.at[it], dev(s, y, 1 - k)
        )
        exchange.start()
        exchange.wait()
        grand = jnp.sum(mtot[it, 0] + mtot[it, 1])
        return jnp.full((8, 128), CELLS / grand, F32)

    def p_wait(src):
        src_dev = dev(src // 4, src % 4, k)

        @pl.when(src != me)
        def _():
            remote(
                prf.at[src], prf.at[src], qs_sem.at[src, 0], qr_sem.at[src, 0], src_dev
            ).wait_recv()
            remote(
                prp.at[src], prp.at[src], qs_sem.at[src, 1], qr_sem.at[src, 1], src_dev
            ).wait_recv()

    def update_group(n):
        src_s = partner_at((n // 4) * 2, 3)
        return ((y + 4 - n % 4) % 4) * 8 + src_s // 2

    def update(scale, n, _):
        group = update_group(n)
        ys = group // 8
        even = ((group % 8) * 2) * 4 + ys
        odd = even + 4
        p_wait(even)
        p_wait(odd)
        a, b = prp[even].astype(F32), prp[odd].astype(F32)
        mid_top = jnp.where(mask48, a, swap(b))
        mid_bottom = jnp.where(mask48, swap(a), b)
        mid = jnp.concatenate(
            [mid_top.reshape(3, 16, 128), mid_bottom.reshape(3, 16, 128)], axis=1
        ).reshape(96, 128)
        first, third = prf[even].astype(F32), prf[odd].astype(F32)
        for t, value in enumerate((first.reshape(96, 128), mid, third.reshape(96, 128))):
            col = pl.multiple_of((group % 8) * 384 + t * 128, 128)
            before = prior_r[ys, :, :, pl.ds(col, 128)].reshape(96, 128)
            now = (MIX * value + (1.0 - MIX) * before) * scale
            xr[group * 3 + t, pl.ds(pl.multiple_of(k * 96, 16), 96), :] = now.astype(BF)

        @pl.when(n > 0)
        def _():
            forward_state(update_group(n - 1)).start()

        return 0

    second_stage()
    stage5(0)
    for cp in gather_copies:
        cp.wait_send()
    m1 = first_stage(False, 0)
    scale = m1[0:1, :]
    lax.fori_loop(0, 32, functools.partial(update, scale), 0)
    forward_state(update_group(31)).start()

    def p_sent(i, _):
        p_copies(i, False, end_send)
        return 0

    lax.fori_loop(0, 16, p_sent, 0)

    second_stage()
    mout[...] = first_stage(True, 1)

    def p_last(i, _):
        p_copies(i, True, end_send)
        return 0

    lax.fori_loop(0, 16, p_last, 0)

    def out_wait(i, _):
        src = (s + i) % 16
        remote(
            outf.at[src], outf.at[src], os_sem.at[src, 0], or_sem.at[src, 0], dev(src, y, k)
        ).wait_recv()
        remote(
            outp.at[src], outp.at[src], os_sem.at[src, 1], or_sem.at[src, 1], dev(src, y, k)
        ).wait_recv()
        return 0

    lax.fori_loop(1, 16, out_wait, 0)


def run_main(prior, t1, t2, c1, c2):
    any_spec = pl.BlockSpec(memory_space=pl.ANY)
    vmem = pl.BlockSpec(memory_space=pltpu.VMEM)
    dma = pltpu.SemaphoreType.DMA
    scratch = [
        pltpu.VMEM((4, 3, 32, 3072), F32),
        pltpu.VMEM((30720, 128), BF),
        pltpu.VMEM((4, 7680, 128), BF),
        pltpu.VMEM((96, 208, 128), BF),
        pltpu.VMEM((96, 128, 256), BF),
        pltpu.VMEM((48, 128, 128), BF),
        pltpu.VMEM((32, 2, 3, 32, 128), BF),
        pltpu.VMEM((32, 3, 32, 128), BF),
        pltpu.VMEM((48, 128, 128), BF),
        pltpu.VMEM((16, 4, 48, 128), BF),
        pltpu.VMEM((3, 128, 128), F32),
        pltpu.VMEM((64, 3, 32, 128), BF),
        pltpu.VMEM((64, 48, 128), BF),
        pltpu.VMEM((2, 64, 1, 128), F32),
        pltpu.VMEM((2, 1, 128), F32),
        pltpu.VMEM((8, 128), F32),
        pltpu.VMEM((2, 2, 1, 128), F32),
        pltpu.VMEM((8, 128), F32),
        pltpu.VMEM((16, 8, 128), jnp.int32),
        pltpu.VMEM((4, 24, 128), jnp.int32),
        pltpu.SMEM((16, 8, 128), jnp.int32),
        pltpu.SMEM((4, 24, 128), jnp.int32),
        dma((7,)), dma((4,)), dma((4,)), dma((20,)), dma((20,)), dma((4,)), dma((4,)),
        dma((2, 2, 5, 4)), dma((2, 2, 5, 4)), dma((32,)), dma((32,)),
        dma((32, 2, 2)), dma((64, 2)), dma((64, 2)), dma((64, 2)),
        dma((64, 2)), dma((64, 2)), dma((16, 2)), dma((16, 2)),
        dma((64,)), dma((64,)), dma((2,)), dma((2,)),
    ]
    return pl.pallas_call(
        main_kernel,
        out_shape=(
            jax.ShapeDtypeStruct((16, 3, 128, 128), BF),
            jax.ShapeDtypeStruct((16, 4, 48, 128), BF),
            jax.ShapeDtypeStruct((8, 128), F32),
        ),
        in_specs=[any_spec, any_spec, any_spec, vmem, vmem],
        out_specs=(any_spec, any_spec, vmem),
        scratch_shapes=scratch,
        compiler_params=pltpu.CompilerParams(
            collective_id=0, has_side_effects=True, vmem_limit_bytes=60 << 20
        ),
        name="align",
    )(prior, t1, t2, c1, c2)


def combine_kernel(pf, pp, m, prior, out):
    mask = half_lanes((192, 128))
    scale = m[0:1, :]
    a, b = pp[0].astype(F32), pp[1].astype(F32)
    mid = jnp.concatenate([jnp.where(mask, a, swap(b)), jnp.where(mask, swap(a), b)], axis=0)
    for t, value in enumerate((pf[0].astype(F32), mid, pf[1].astype(F32))):
        cols = slice(t * 128, (t + 1) * 128)
        out[:, cols] = (MIX * value + (1.0 - MIX) * prior[:, cols]) * scale


def combine(pf, pp, m, prior):
    return pl.pallas_call(
        combine_kernel,
        grid=(8,),
        out_shape=jax.ShapeDtypeStruct((384, 3072), F32),
        in_specs=[
            pl.BlockSpec((2, 384, 128), lambda i: (i, 0, 0)),
            pl.BlockSpec((2, 192, 128), lambda i: (i, 0, 0)),
            pl.BlockSpec((8, 128), lambda i: (0, 0)),
            pl.BlockSpec((384, 384), lambda i: (0, i)),
        ],
        out_specs=pl.BlockSpec((384, 384), lambda i: (0, i)),
        name="combine",
    )(pf, pp, m, prior)


def local(prior_scores, tiles_first, columns_first, tiles_second, columns_second):
    t1 = tiles_first.reshape(1920, 128)
    t2 = tiles_second.reshape(15360, 128)
    c1 = jnp.pad(columns_first.astype(jnp.int32), ((0, 5), (0, 123)))
    c2 = jnp.pad(columns_second.astype(jnp.int32), ((0, 0), (0, 123)))
    pf, pp, m = run_main(prior_scores.reshape(3, 128, 3072), t1, t2, c1, c2)
    return combine(
        pf.reshape(16, 384, 128), pp.reshape(16, 192, 128), m, prior_scores
    )


def solution(mesh):
    return jax.shard_map(
        local,
        mesh=mesh,
        in_specs=(
            P("row", "col"),
            P("row", None, None, None),
            P("row", None),
            P("col", None, None, None),
            P("col", None),
        ),
        out_specs=P("row", "col"),
        check_vma=False,
    )
```

```python
import functools

import jax
import jax.numpy as jnp
from jax import lax
from jax.experimental import pallas as pl
from jax.experimental.pallas import tpu as pltpu
from jax.sharding import PartitionSpec as P

MESH = pl.DeviceIdType.MESH
BF = jnp.bfloat16
F32 = jnp.float32
MIX = 0.8
CELLS = float(12288 * 12288)
HELD = 8
NT = (((1,), (1,)), ((), ()))
NN = (((1,), (0,)), ((), ()))


def half_lanes(shape):
    return lax.broadcasted_iota(jnp.int32, shape, 1) < 64


def swap(value):
    return pltpu.roll(value, 64, 1)


def main_kernel(
    prior, t1, t2, c1, c2,
    outf, outp, mout,
    prior_r, a1, a2, xr, zc, zpk, zsend, zspk, pfull, ppk, ph, prf, prp,
    mbuf, msend, mpart, mtot, macc, c1p, c2p, c1g, c2g, c1s, c2s,
    lsem, ss, sr, gr_sem, zr_sem, ff_sem, qr_sem,
):
    row = lax.axis_index("row")
    y = lax.axis_index("col")
    k = row % 2
    s = row // 2
    x = s % 4
    z = s // 4
    me = s * 4 + y

    def dev(s_, y_, k_):
        return {"row": s_ * 2 + k_, "col": y_}

    def remote(src, dst, ssem, rsem, target):
        return pltpu.make_async_remote_copy(
            src_ref=src, dst_ref=dst, send_sem=ssem, recv_sem=rsem,
            device_id=target, device_id_type=MESH,
        )

    def all_of(ref, number):
        return remote(ref, ref, ss.at[number], sr.at[number], dev(s, y, 1 - k))

    def rows_of(count, send, recv):
        ref = a1.at[pl.ds(0, count)]
        return remote(ref, ref, send, recv, dev(s, y, 1 - k))

    barrier = pltpu.get_barrier_semaphore()

    def greet(i, _):
        other = (row * 4 + y + i) % 128
        pl.semaphore_signal(
            barrier, inc=1, device_id={"row": other // 4, "col": other % 4}, device_id_type=MESH
        )
        return 0

    load1 = pltpu.make_async_copy(t1, a1.at[pl.ds(s * 1920, 1920)], lsem.at[0])
    load1.start()
    load2 = pltpu.make_async_copy(t2.at[pl.ds(k * 7680, 7680)], a2.at[0], lsem.at[1])
    load2.start()
    load3 = pltpu.make_async_copy(
        prior.at[:, pl.ds(pl.multiple_of(y * 32, 32), 32), :], prior_r.at[y], lsem.at[2]
    )
    load3.start()
    lax.fori_loop(1, 128, greet, 0)
    c1p[0:3, 0:5] = c1[...]
    c2p[:, 0:5] = c2[...]
    c1g[s] = c1p[...]
    c2g[y] = c2p[...]
    xr[:, 192:208, :] = jnp.ones((96, 16, 128), BF)
    pl.semaphore_wait(barrier, 127)

    for d in (1, 3, 2):
        yd = (y + d) % 4
        cp = remote(
            t2.at[pl.ds(k * 7680 + s * 480, 480)],
            a2.at[(4 - d) % 4, pl.ds(s * 480, 480)],
            ss.at[2], sr.at[2], dev(s, yd, k),
        )
        cp.start()
        cc = remote(c2p, c2g.at[y], ss.at[1], sr.at[1], dev(s, yd, k))
        cc.start()

    XP, XM = (z * 4 + (x + 1) % 4), (z * 4 + (x + 3) % 4)
    ZP, ZM = (((z + 1) % 4) * 4 + x), (((z + 3) % 4) * 4 + x)

    def region(kind, origin, part):
        if kind == 0:
            off, size = ((0, 480), (480, 480), (960, 480), (1440, 480), (0, 960), (960, 960))[part]
            return a1.at[pl.ds(pl.multiple_of(origin * 1920 + off, 16), size)]
        off, size = ((0, 128), (128, 112), (240, 128), (368, 112), (0, 240), (240, 240))[part]
        return a2.at[pl.ds(1, 3), pl.ds(pl.multiple_of(origin * 480 + off, 16), size)]

    def nbr(axis, up):
        return (XP if up else XM) if axis == 0 else (ZP if up else ZM)

    def shifted(axis, origin, delta):
        ox, oz = origin % 4, origin // 4
        if axis == 0:
            return oz * 4 + (ox + delta) % 4
        return ((oz + delta) % 4) * 4 + ox

    def hop(kind, half, group, slot, origin, part, axis, up):
        cp = remote(
            region(kind, origin, part), region(kind, origin, part),
            ss.at[4 + kind], gr_sem.at[kind, half, group, slot],
            dev(nbr(axis, up), y, k),
        )
        cp.start()

    def landed(kind, half, group, slot, origin, part):
        cp = remote(
            region(kind, origin, part), region(kind, origin, part),
            ss.at[4 + kind], gr_sem.at[kind, half, group, slot],
            dev(nbr(0, True), y, k),
        )
        cp.wait_recv()

    def whole(half):
        return 4 + half

    def ring_start(kind, half, group, origin, axis):
        hop(kind, half, group, 0, origin, whole(half), axis, True)
        hop(kind, half, group, 1, origin, whole(half), axis, False)

    def ring_relay(kind, half, group, base, axis):
        low, high = shifted(axis, base, 3), shifted(axis, base, 1)
        landed(kind, half, group, 0, low, whole(half))
        hop(kind, half, group, 2, low, 2 * half, axis, True)
        landed(kind, half, group, 1, high, whole(half))
        hop(kind, half, group, 3, high, 2 * half + 1, axis, False)

    def ring_end(kind, half, group, base, axis):
        far = shifted(axis, base, 2)
        landed(kind, half, group, 2, far, 2 * half)
        landed(kind, half, group, 3, far, 2 * half + 1)

    def stage1(kind):
        for half in (0, 1):
            ring_start(kind, half, 0, s, half)
        for half in (0, 1):
            ring_start(kind, half, 1, s, 1 - half)

    def stage2(kind):
        for half in (0, 1):
            ring_relay(kind, half, 0, s, half)
            for g, delta in ((2, 3), (3, 1)):
                ring_start(kind, half, g, shifted(half, s, delta), 1 - half)

    def stage3(kind):
        for half in (0, 1):
            ring_end(kind, half, 0, s, half)
            ring_start(kind, half, 4, shifted(half, s, 2), 1 - half)

    def stage4(kind):
        for g, delta in ((1, 0), (2, 3), (3, 1), (4, 2)):
            for half in (0, 1):
                ring_relay(kind, half, g, shifted(half, s, delta), 1 - half)

    def stage5(kind):
        for g, delta in ((1, 0), (2, 3), (3, 1), (4, 2)):
            for half in (0, 1):
                ring_end(kind, half, g, shifted(half, s, delta), 1 - half)

    load1.wait()
    stage1(0)
    for d in (1, 3, 2):
        yd = (y + d) % 4
        cp = remote(
            prior.at[:, pl.ds(pl.multiple_of(yd * 32, 32), 32), :], prior_r.at[y],
            ss.at[3], sr.at[3], dev(s, yd, k),
        )
        cp.start()

    def send_columns(i, _):
        remote(
            c1p, c1g.at[s], ss.at[0], sr.at[0], dev((s + i) % 16, y, k)
        ).start()
        return 0

    lax.fori_loop(1, 16, send_columns, 0)

    all_of(a2.at[pl.ds(1, 3), pl.ds(0, 480)], 2).wait()
    stage1(1)
    stage2(0)
    stage2(1)
    stage3(0)
    stage3(1)
    load3.wait()
    load2.wait()

    all_of(c2g.at[pl.ds(0, 3)], 1).wait()
    all_of(c1g.at[pl.ds(0, 15)], 0).wait()
    cps = [
        pltpu.make_async_copy(c1g, c1s, lsem.at[3]),
        pltpu.make_async_copy(c2g, c2s, lsem.at[4]),
    ]
    for cp in cps:
        cp.start()
    for cp in cps:
        cp.wait()

    stage4(1)
    stage4(0)
    all_of(prior_r.at[pl.ds(0, 3)], 3).wait()

    mask96 = half_lanes((96, 128))
    mask48 = half_lanes((48, 128))

    def forward_state(group):
        return remote(
            xr.at[pl.ds(group * 3, 3), pl.ds(k * 96, 96)],
            xr.at[pl.ds(group * 3, 3), pl.ds(k * 96, 96)],
            ss.at[6], sr.at[6], dev(s, y, 1 - k),
        )

    def state_wait():
        all_of(xr.at[:, pl.ds(pl.multiple_of((1 - k) * 96, 16), 96)], 6).wait()

    macc[...] = jnp.zeros((8, 128), F32)

    def convert(group, _):
        ys = group // 8
        for t in range(3):
            col = pl.multiple_of((group % 8) * 384 + t * 128, 128)
            value = prior_r[ys, :, :, pl.ds(col, 128)].reshape(96, 128)
            macc[...] += jnp.sum(value.reshape(12, 8, 128), axis=0)
            xr[group * 3 + t, pl.ds(pl.multiple_of(k * 96, 16), 96), :] = value.astype(BF)

        @pl.when(group > 0)
        def _():
            forward_state(group - 1).start()

        return 0

    lax.fori_loop(0, 32, convert, 0)
    forward_state(31).start()
    stage5(1)

    def z_places(src_s, src_y, p):
        return (
            (
                pl.ds((src_s * 2 + p) * 3, 3),
                pl.ds(pl.multiple_of(src_y * 32, 32), 32),
                pl.ds(0, 128),
            ),
            (
                p,
                pl.ds(src_s * 3, 3),
                pl.ds(pl.multiple_of(src_y * 16, 16), 16),
                pl.ds(0, 128),
            ),
        )

    ZG = x + 2 * z

    def z_copies(i):
        yd = (y + i * (1 + 2 * k)) % 4
        g = (i // 4 + ZG) % 4
        for d in range(2):
            sd = k * 8 + g * 2 + d
            slot = yd * 8 + g * 2 + d
            for p in range(2):
                self_part = jnp.logical_and(jnp.logical_and(sd == s, yd == y), k == p)
                full_at, packed_at = z_places(s, y, p)
                full = remote(
                    zsend.at[slot, p], zc.at[full_at],
                    ss.at[7], zr_sem.at[s], dev(sd, yd, p),
                )
                packed = remote(
                    zspk.at[slot, :, pl.ds(p * 16, 16), :], zpk.at[packed_at],
                    ss.at[7], zr_sem.at[s], dev(sd, yd, p),
                )

                @pl.when(jnp.logical_not(self_part))
                def _():
                    full.start()
                    packed.start()

                @pl.when(self_part)
                def _():
                    zc[full_at] = zsend[slot, p]
                    zpk[packed_at] = zspk[slot, :, p * 16 : p * 16 + 16, :]

    def z_compute(i, _):
        yd = (y + i * (1 + 2 * k)) % 4
        g = (i // 4 + ZG) % 4
        yr = (i * (1 + 2 * k)) % 4
        values = []
        for t in range(3):
            jl = g * 3 + t
            acc = None
            for slot in range(5):
                c = c2s[yd, k * 12 + jl, slot]
                tile = a2[yr, pl.ds(pl.multiple_of((jl * 5 + slot) * 128, 128), 128), :]
                part = lax.dot_general(xr[c], tile, NT, preferred_element_type=F32)
                acc = part if acc is None else acc + part
            inv = 1.0 / acc[192:193, :]
            values.append(acc[0:192, :] * inv)
        out = yd * 8 + g * 2
        for p in range(2):
            rows = slice(p * 96, p * 96 + 96)
            zsend[out, p] = values[0][rows].astype(BF).reshape(3, 32, 128)
            zsend[out + 1, p] = values[2][rows].astype(BF).reshape(3, 32, 128)
        top, bottom = values[1][0:96], values[1][96:192]
        even = jnp.where(mask96, top, swap(bottom))
        odd = jnp.where(mask96, swap(top), bottom)
        zspk[out] = even.astype(BF).reshape(3, 32, 128)
        zspk[out + 1] = odd.astype(BF).reshape(3, 32, 128)

        @pl.when(i > 0)
        def _():
            z_copies(i - 1)

        return 0

    def z_forward(src_s, p):
        full, packed = pl.ds((src_s * 2 + p) * 3, 3), pl.ds(src_s * 3, 3)
        return [
            remote(ref, ref, ss.at[8], ff_sem.at[src_s], dev(s, y, 1 - k))
            for ref in (zc.at[full, :, pl.ds(0, 128)], zpk.at[p, packed])
        ]

    def z_source(n):
        c = ((s % 8) // 2 + 4 - n // 16) % 4
        r = (n // 4) % 4
        xs = c % 2 + 2 * (r % 2)
        zs = ((c + 4 - xs) // 2) % 2 + 2 * (r // 2)
        return zs * 4 + xs

    def z_receive(i, _):
        src_s = z_source(i * 4)
        own = jnp.logical_and(src_s == s, s // 8 == k)

        @pl.when(own)
        def _():
            rows_of(432, ss.at[7], zr_sem.at[src_s]).wait_recv()

        @pl.when(jnp.logical_not(own))
        def _():
            rows_of(576, ss.at[7], zr_sem.at[src_s]).wait_recv()

        for cp in z_forward(src_s, k):
            cp.start()
        return 0

    def z_finish(i, _):
        rows_of(576, ss.at[8], ff_sem.at[z_source(i * 4)]).wait_recv()
        return 0

    def z_unpack(n, _):
        i = z_source((n // 3) * 4) * 3 + n % 3
        parts = [zpk[p, i].astype(F32).reshape(4, 16, 128) for p in range(2)]
        packed = jnp.concatenate(parts, axis=1).reshape(128, 128)
        lane = lax.broadcasted_iota(jnp.int32, (128, 128), 1)
        fill = jnp.where(lane == 64, 1.0, 0.0).astype(F32)
        block = (i // 3) * 6 + i % 3
        zc[block, :, 128:256] = jnp.where(lane < 64, packed, fill).astype(BF)
        zc[block + 3, :, 128:256] = jnp.where(lane < 64, swap(packed), fill).astype(BF)
        return 0

    def second_stage():
        state_wait()
        lax.fori_loop(0, 16, z_compute, 0)
        z_copies(15)
        for phase in range(5):
            if phase < 4:
                lax.fori_loop(phase * 4, phase * 4 + 4, z_receive, 0)
            if phase > 0:
                lax.fori_loop(phase * 4 - 4, phase * 4, z_finish, 0)
                lax.fori_loop(phase * 12 - 12, phase * 12, z_unpack, 0)

        own = s // 8 == k

        @pl.when(own)
        def _():
            rows_of(32 * 288 - 144, ss.at[7], sr.at[4]).wait_send()

        @pl.when(jnp.logical_not(own))
        def _():
            rows_of(32 * 288, ss.at[7], sr.at[4]).wait_send()

        rows_of(16 * 576, ss.at[8], sr.at[4]).wait_send()

    def partner_at(i, sign):
        j = i // 2
        dz = (j % 4) * (1 + 2 * k) * sign
        xa = (x + 2 * ((j // 4 + j) % 2)) % 4
        return ((z + dz) % 4) * 4 + xa + (i % 2) * (1 - 2 * (xa % 2))

    def target(i):
        return partner_at(i, 1)

    def p_copies(i, last):
        sd = target(i)
        if last:
            full = (pfull.at[pl.ds(sd * 3, 3)], outf.at[s])
            packed = (ppk.at[sd], outp.at[s])
            pair = [
                remote(*full, ss.at[9], sr.at[9], dev(sd, y, k)),
                remote(*packed, ss.at[9], sr.at[9], dev(sd, y, k)),
            ]
            mine = [
                pltpu.make_async_copy(*full, lsem.at[5]),
                pltpu.make_async_copy(*packed, lsem.at[6]),
            ]

            @pl.when(sd != s)
            def _():
                for cp in pair:
                    cp.start()

            @pl.when(sd == s)
            def _():
                for cp in mine:
                    cp.start()

            return
        for step in range(4):
            yd = (y + step) % 4
            pair = [
                remote(
                    pfull.at[pl.ds(sd * 3, 3), pl.ds(pl.multiple_of(yd * 32, 32), 32)], prf.at[me],
                    ss.at[9], qr_sem.at[y * 8 + s // 2], dev(sd, yd, k),
                ),
                remote(
                    ppk.at[sd, yd], prp.at[me],
                    ss.at[9], qr_sem.at[y * 8 + s // 2], dev(sd, yd, k),
                ),
            ]

            if step > 0:
                for cp in pair:
                    cp.start()
                continue

            @pl.when(sd != s)
            def _():
                for cp in pair:
                    cp.start()

            @pl.when(sd == s)
            def _():
                prf[me] = pfull[pl.ds(sd * 3, 3), pl.ds(pl.multiple_of(y * 32, 32), 32), :]
                prp[me] = ppk[sd, y]

    def p_compute(last, i, _):
        sd = target(i)
        for t in range(3):
            acc = None
            for slot in range(5):
                c = c1s[sd, t, slot]
                tile = a1[pl.ds(pl.multiple_of((sd * 15 + t * 5 + slot) * 128, 128), 128), :]
                part = lax.dot_general(
                    tile, zc[c], NN, preferred_element_type=F32
                )
                acc = part if acc is None else acc + part
            inv = 1.0 / acc[:, 192:193]
            first = (acc[:, 0:128] * inv).astype(BF)
            second = (acc[:, 128:256] * inv).astype(BF).astype(F32)
            second = jnp.where(half_lanes((128, 128)), second, 0.0)
            total = first.astype(F32) + second
            mpart[...] += jnp.sum(total.reshape(16, 8, 128), axis=0)
            pfull[sd * 3 + t] = first
            ph[t] = second
        for yd in range(4):
            if last:
                flat = ph[...].reshape(384, 128)
                low = flat[yd * 48 : yd * 48 + 48]
                high = flat[192 + yd * 48 : 240 + yd * 48]
            else:
                low = ph[:, yd * 32 : yd * 32 + 16, :].reshape(48, 128)
                high = ph[:, yd * 32 + 16 : yd * 32 + 32, :].reshape(48, 128)
            ppk[sd, yd] = (low + swap(high)).astype(BF)

        @pl.when(jnp.logical_and(i > 0, i <= HELD))
        def _():
            p_copies(i - 1, last)

        return 0

    def first_stage(last, it):
        mpart[...] = jnp.zeros((8, 128), F32)
        lax.fori_loop(0, 16, functools.partial(p_compute, last), 0)
        mine = jnp.sum(MIX * mpart[...] + (1.0 - MIX) * macc[...], axis=0, keepdims=True)
        mbuf[it, me] = mine
        msend[it] = mine

        def total_copy(i, src, dst):
            return remote(
                msend.at[it], mbuf.at[it, src], ss.at[10], sr.at[10], dev(dst // 4, dst % 4, k)
            )

        def total_send(i, _):
            total_copy(i, me, (me + i) % 64).start()
            return 0

        def late(i, _):
            p_copies(i, last)
            return 0

        lax.fori_loop(1, 64, total_send, 0)
        lax.fori_loop(HELD, 16, late, 0)
        all_of(mbuf.at[it, pl.ds(0, 63)], 10).wait()
        mtot[it, 0] = jnp.sum(mbuf[it], axis=0)
        exchange = remote(
            mtot.at[it, 0], mtot.at[it, 1], ss.at[11], sr.at[11], dev(s, y, 1 - k)
        )
        exchange.start()
        exchange.wait()
        grand = jnp.sum(mtot[it, 0] + mtot[it, 1])
        return jnp.full((8, 128), CELLS / grand, F32)

    def p_wait(group):
        own = group == y * 8 + s // 2

        @pl.when(own)
        def _():
            rows_of(144, ss.at[9], qr_sem.at[group]).wait_recv()

        @pl.when(jnp.logical_not(own))
        def _():
            rows_of(288, ss.at[9], qr_sem.at[group]).wait_recv()

    def update_group(n):
        src_s = partner_at((n // 4) * 2, 3)
        return ((y + 4 - n % 4) % 4) * 8 + src_s // 2

    def update(scale, n, _):
        group = update_group(n)
        ys = group // 8
        even = ((group % 8) * 2) * 4 + ys
        odd = even + 4
        p_wait(group)
        a, b = prp[even].astype(F32), prp[odd].astype(F32)
        mid_top = jnp.where(mask48, a, swap(b))
        mid_bottom = jnp.where(mask48, swap(a), b)
        mid = jnp.concatenate(
            [mid_top.reshape(3, 16, 128), mid_bottom.reshape(3, 16, 128)], axis=1
        ).reshape(96, 128)
        first, third = prf[even].astype(F32), prf[odd].astype(F32)
        for t, value in enumerate((first.reshape(96, 128), mid, third.reshape(96, 128))):
            col = pl.multiple_of((group % 8) * 384 + t * 128, 128)
            before = prior_r[ys, :, :, pl.ds(col, 128)].reshape(96, 128)
            now = (MIX * value + (1.0 - MIX) * before) * scale
            xr[group * 3 + t, pl.ds(pl.multiple_of(k * 96, 16), 96), :] = now.astype(BF)

        @pl.when(n > 0)
        def _():
            forward_state(update_group(n - 1)).start()

        return 0

    second_stage()
    stage5(0)
    rows_of(15 * 1920, ss.at[4], sr.at[4]).wait_send()
    rows_of(15 * 1440, ss.at[5], sr.at[4]).wait_send()
    m1 = first_stage(False, 0)
    scale = m1[0:1, :]
    lax.fori_loop(0, 32, functools.partial(update, scale), 0)
    forward_state(update_group(31)).start()

    rows_of(63 * 144, ss.at[9], sr.at[4]).wait_send()

    second_stage()
    mout[...] = first_stage(True, 1)

    rows_of(15 * 576, ss.at[9], sr.at[9]).wait()
    pltpu.make_async_copy(pfull.at[pl.ds(s * 3, 3)], outf.at[s], lsem.at[5]).wait()
    pltpu.make_async_copy(ppk.at[s], outp.at[s], lsem.at[6]).wait()


def run_main(prior, t1, t2, c1, c2):
    any_spec = pl.BlockSpec(memory_space=pl.ANY)
    vmem = pl.BlockSpec(memory_space=pltpu.VMEM)
    dma = pltpu.SemaphoreType.DMA
    scratch = [
        pltpu.VMEM((4, 3, 32, 3072), F32),
        pltpu.VMEM((30720, 128), BF),
        pltpu.VMEM((4, 7680, 128), BF),
        pltpu.VMEM((96, 208, 128), BF),
        pltpu.VMEM((96, 128, 256), BF),
        pltpu.VMEM((2, 48, 64, 128), BF),
        pltpu.VMEM((32, 2, 3, 32, 128), BF),
        pltpu.VMEM((32, 3, 32, 128), BF),
        pltpu.VMEM((48, 128, 128), BF),
        pltpu.VMEM((16, 4, 48, 128), BF),
        pltpu.VMEM((3, 128, 128), F32),
        pltpu.VMEM((64, 3, 32, 128), BF),
        pltpu.VMEM((64, 48, 128), BF),
        pltpu.VMEM((2, 64, 1, 128), F32),
        pltpu.VMEM((2, 1, 128), F32),
        pltpu.VMEM((8, 128), F32),
        pltpu.VMEM((2, 2, 1, 128), F32),
        pltpu.VMEM((8, 128), F32),
        pltpu.VMEM((8, 128), jnp.int32),
        pltpu.VMEM((24, 128), jnp.int32),
        pltpu.VMEM((16, 8, 128), jnp.int32),
        pltpu.VMEM((4, 24, 128), jnp.int32),
        pltpu.SMEM((16, 8, 128), jnp.int32),
        pltpu.SMEM((4, 24, 128), jnp.int32),
        dma((7,)), dma((12,)), dma((12,)), dma((2, 2, 5, 4)), dma((16,)), dma((16,)), dma((32,)),
    ]
    return pl.pallas_call(
        main_kernel,
        out_shape=(
            jax.ShapeDtypeStruct((16, 3, 128, 128), BF),
            jax.ShapeDtypeStruct((16, 4, 48, 128), BF),
            jax.ShapeDtypeStruct((8, 128), F32),
        ),
        in_specs=[any_spec, any_spec, any_spec, vmem, vmem],
        out_specs=(any_spec, any_spec, vmem),
        scratch_shapes=scratch,
        compiler_params=pltpu.CompilerParams(
            collective_id=0, has_side_effects=True, vmem_limit_bytes=60 << 20
        ),
        name="align",
    )(prior, t1, t2, c1, c2)


def combine_kernel(pf, pp, m, prior, out):
    mask = half_lanes((192, 128))
    scale = m[0:1, :]
    a, b = pp[0].astype(F32), pp[1].astype(F32)
    mid = jnp.concatenate([jnp.where(mask, a, swap(b)), jnp.where(mask, swap(a), b)], axis=0)
    for t, value in enumerate((pf[0].astype(F32), mid, pf[1].astype(F32))):
        cols = slice(t * 128, (t + 1) * 128)
        out[:, cols] = (MIX * value + (1.0 - MIX) * prior[:, cols]) * scale


def combine(pf, pp, m, prior):
    return pl.pallas_call(
        combine_kernel,
        grid=(8,),
        out_shape=jax.ShapeDtypeStruct((384, 3072), F32),
        in_specs=[
            pl.BlockSpec((2, 384, 128), lambda i: (i, 0, 0)),
            pl.BlockSpec((2, 192, 128), lambda i: (i, 0, 0)),
            pl.BlockSpec((8, 128), lambda i: (0, 0)),
            pl.BlockSpec((384, 384), lambda i: (0, i)),
        ],
        out_specs=pl.BlockSpec((384, 384), lambda i: (0, i)),
        name="combine",
    )(pf, pp, m, prior)


def local(prior_scores, tiles_first, columns_first, tiles_second, columns_second):
    t1 = tiles_first.reshape(1920, 128)
    t2 = tiles_second.reshape(15360, 128)
    pf, pp, m = run_main(
        prior_scores.reshape(3, 128, 3072), t1, t2, columns_first, columns_second
    )
    return combine(
        pf.reshape(16, 384, 128), pp.reshape(16, 192, 128), m, prior_scores
    )


def solution(mesh):
    return jax.shard_map(
        local,
        mesh=mesh,
        in_specs=(
            P("row", "col"),
            P("row", None, None, None),
            P("row", None),
            P("col", None, None, None),
            P("col", None),
        ),
        out_specs=P("row", "col"),
        check_vma=False,
    )
```

```python
import functools

import jax
import jax.numpy as jnp
from jax import lax
from jax.experimental import pallas as pl
from jax.experimental.pallas import tpu as pltpu
from jax.sharding import PartitionSpec as P

MESH = pl.DeviceIdType.MESH
BF = jnp.bfloat16
F32 = jnp.float32
MIX = 0.8
CELLS = float(12288 * 12288)
HELD = 8
CQ = 2
NT = (((1,), (1,)), ((), ()))
NN = (((1,), (0,)), ((), ()))


def half_lanes(shape):
    return lax.broadcasted_iota(jnp.int32, shape, 1) < 64


def swap(value):
    return pltpu.roll(value, 64, 1)


def main_kernel(
    prior, t1, t2, c1, c2,
    outf, outp, mout,
    prior_r, a1, a2, xr, zc, zpk, zsend, zspk, pfull, ppk, ph, prf, prp,
    mbuf, msend, mpart, mtot, macc, c1p, c2p, c1g, c2g, c1s, c2s,
    rounds, lsem, ss, sr, gr_sem, zr_sem, ff_sem, qr_sem,
):
    row = lax.axis_index("row")
    y = lax.axis_index("col")
    k = row % 2
    s = row // 2
    x = s % 4
    z = s // 4
    me = s * 4 + y

    def dev(s_, y_, k_):
        return {"row": s_ * 2 + k_, "col": y_}

    def remote(src, dst, ssem, rsem, target):
        return pltpu.make_async_remote_copy(
            src_ref=src, dst_ref=dst, send_sem=ssem, recv_sem=rsem,
            device_id=target, device_id_type=MESH,
        )

    def all_of(ref, number):
        return remote(ref, ref, ss.at[number], sr.at[number], dev(s, y, 1 - k))

    def rows_of(count, send, recv):
        ref = a1.at[pl.ds(0, count)]
        return remote(ref, ref, send, recv, dev(s, y, 1 - k))

    x_line = [dev(z * 4 + (x + d) % 4, y, k) for d in (1, 2, 3)]
    z_line = [dev(((z + d) % 4) * 4 + x, y, k) for d in (1, 2, 3)]
    y_line = [dev(s, (y + d) % 4, k) for d in (1, 2, 3)]
    pair_line = [dev(s, y, 1 - k)]

    def greet(sem, peers):
        for peer in peers:
            pl.semaphore_signal(sem, inc=1, device_id=peer, device_id_type=MESH)

    barrier = pltpu.get_barrier_semaphore()
    greet(barrier, x_line + z_line + y_line + pair_line)

    load1 = pltpu.make_async_copy(t1, a1.at[pl.ds(s * 1920, 1920)], lsem.at[0])
    load1.start()
    load2 = pltpu.make_async_copy(t2.at[pl.ds(k * 7680, 7680)], a2.at[0], lsem.at[1])
    load2.start()
    load3 = pltpu.make_async_copy(
        prior.at[:, pl.ds(pl.multiple_of(y * 32, 32), 32), :], prior_r.at[y], lsem.at[2]
    )
    load3.start()
    c1p[0:3, 0:5] = c1[...]
    c2p[:, 0:5] = c2[...]
    c1g[s] = c1p[...]
    c2g[y] = c2p[...]
    xr[:, 192:208, :] = jnp.ones((96, 16, 128), BF)
    pl.semaphore_wait(barrier, 10)
    greet(rounds.at[0], x_line)

    for d in (1, 3, 2):
        yd = (y + d) % 4
        cp = remote(
            t2.at[pl.ds(k * 7680 + s * 480, 480)],
            a2.at[(4 - d) % 4, pl.ds(s * 480, 480)],
            ss.at[2], sr.at[2], dev(s, yd, k),
        )
        cp.start()
        cc = remote(c2p, c2g.at[y], ss.at[1], sr.at[1], dev(s, yd, k))
        cc.start()

    XP, XM = (z * 4 + (x + 1) % 4), (z * 4 + (x + 3) % 4)
    ZP, ZM = (((z + 1) % 4) * 4 + x), (((z + 3) % 4) * 4 + x)

    def region(kind, origin, part):
        if kind == 0:
            off, size = ((0, 480), (480, 480), (960, 480), (1440, 480), (0, 960), (960, 960))[part]
            return a1.at[pl.ds(pl.multiple_of(origin * 1920 + off, 16), size)]
        off, size = ((0, 128), (128, 112), (240, 128), (368, 112), (0, 240), (240, 240))[part]
        return a2.at[pl.ds(1, 3), pl.ds(pl.multiple_of(origin * 480 + off, 16), size)]

    def nbr(axis, up):
        return (XP if up else XM) if axis == 0 else (ZP if up else ZM)

    def shifted(axis, origin, delta):
        ox, oz = origin % 4, origin // 4
        if axis == 0:
            return oz * 4 + (ox + delta) % 4
        return ((oz + delta) % 4) * 4 + ox

    def hop(kind, half, group, slot, origin, part, axis, up):
        cp = remote(
            region(kind, origin, part), region(kind, origin, part),
            ss.at[4 + kind], gr_sem.at[kind, half, group, slot],
            dev(nbr(axis, up), y, k),
        )
        cp.start()

    def landed(kind, half, group, slot, origin, part):
        cp = remote(
            region(kind, origin, part), region(kind, origin, part),
            ss.at[4 + kind], gr_sem.at[kind, half, group, slot],
            dev(nbr(0, True), y, k),
        )
        cp.wait_recv()

    def whole(half):
        return 4 + half

    def ring_start(kind, half, group, origin, axis):
        hop(kind, half, group, 0, origin, whole(half), axis, True)
        hop(kind, half, group, 1, origin, whole(half), axis, False)

    def ring_relay(kind, half, group, base, axis):
        low, high = shifted(axis, base, 3), shifted(axis, base, 1)
        landed(kind, half, group, 0, low, whole(half))
        hop(kind, half, group, 2, low, 2 * half, axis, True)
        landed(kind, half, group, 1, high, whole(half))
        hop(kind, half, group, 3, high, 2 * half + 1, axis, False)

    def ring_end(kind, half, group, base, axis):
        far = shifted(axis, base, 2)
        landed(kind, half, group, 2, far, 2 * half)
        landed(kind, half, group, 3, far, 2 * half + 1)

    def stage1(kind):
        for half in (0, 1):
            ring_start(kind, half, 0, s, half)
        for half in (0, 1):
            ring_start(kind, half, 1, s, 1 - half)

    def stage2(kind):
        for half in (0, 1):
            ring_relay(kind, half, 0, s, half)
            for g, delta in ((2, 3), (3, 1)):
                ring_start(kind, half, g, shifted(half, s, delta), 1 - half)

    def stage3(kind):
        for half in (0, 1):
            ring_end(kind, half, 0, s, half)
            ring_start(kind, half, 4, shifted(half, s, 2), 1 - half)

    def stage4(kind):
        for g, delta in ((1, 0), (2, 3), (3, 1), (4, 2)):
            for half in (0, 1):
                ring_relay(kind, half, g, shifted(half, s, delta), 1 - half)

    def stage5(kind):
        for g, delta in ((1, 0), (2, 3), (3, 1), (4, 2)):
            for half in (0, 1):
                ring_end(kind, half, g, shifted(half, s, delta), 1 - half)

    load1.wait()
    stage1(0)
    for d in (1, 3, 2):
        yd = (y + d) % 4
        cp = remote(
            prior.at[:, pl.ds(pl.multiple_of(yd * 32, 32), 32), :], prior_r.at[y],
            ss.at[3], sr.at[3], dev(s, yd, k),
        )
        cp.start()

    def send_columns(i, _):
        remote(
            c1p, c1g.at[s], ss.at[0], sr.at[0], dev((s + i) % 16, y, k)
        ).start()
        return 0

    pl.semaphore_wait(rounds.at[0], 3)
    greet(rounds.at[1], z_line)
    lax.fori_loop(1, 16, send_columns, 0)

    all_of(a2.at[pl.ds(1, 3), pl.ds(0, 480)], 2).wait()
    stage1(1)
    stage2(1)
    stage2(0)
    stage3(1)
    stage3(0)
    load3.wait()
    load2.wait()

    pl.semaphore_wait(rounds.at[1], 3)
    greet(rounds.at[2], pair_line)

    all_of(c2g.at[pl.ds(0, 3)], 1).wait()
    all_of(c1g.at[pl.ds(0, 15)], 0).wait()
    cps = [
        pltpu.make_async_copy(c1g, c1s, lsem.at[3]),
        pltpu.make_async_copy(c2g, c2s, lsem.at[4]),
    ]
    for cp in cps:
        cp.start()
    for cp in cps:
        cp.wait()

    stage4(1)
    pl.semaphore_wait(rounds.at[2], 1)
    stage4(0)
    all_of(prior_r.at[pl.ds(0, 3)], 3).wait()

    mask96 = half_lanes((96, 128))
    mask48 = half_lanes((48, 128))

    def forward_state(group):
        return remote(
            xr.at[pl.ds(group * 3, 3), pl.ds(k * 96, 96)],
            xr.at[pl.ds(group * 3, 3), pl.ds(k * 96, 96)],
            ss.at[6], sr.at[6], dev(s, y, 1 - k),
        )

    def state_wait():
        all_of(xr.at[:, pl.ds(pl.multiple_of((1 - k) * 96, 16), 96)], 6).wait()

    macc[...] = jnp.zeros((8, 128), F32)

    def convert(group, _):
        ys = group // 8
        for t in range(3):
            col = pl.multiple_of((group % 8) * 384 + t * 128, 128)
            value = prior_r[ys, :, :, pl.ds(col, 128)].reshape(96, 128)
            macc[...] += jnp.sum(value.reshape(12, 8, 128), axis=0)
            xr[group * 3 + t, pl.ds(pl.multiple_of(k * 96, 16), 96), :] = value.astype(BF)

        @pl.when(group > 0)
        def _():
            forward_state(group - 1).start()

        return 0

    lax.fori_loop(0, 32, convert, 0)
    forward_state(31).start()
    stage5(1)

    def z_places(src_s, src_y, p):
        return (
            (
                pl.ds((src_s * 2 + p) * 3, 3),
                pl.ds(pl.multiple_of(src_y * 32, 32), 32),
                pl.ds(0, 128),
            ),
            (
                p,
                pl.ds(src_s * 3, 3),
                pl.ds(pl.multiple_of(src_y * 16, 16), 16),
                pl.ds(0, 128),
            ),
        )

    ZG = x + 2 * z

    def z_copies(i):
        yd = (y + i * (1 + 2 * k)) % 4
        g = (i // 4 + ZG) % 4
        for d in range(2):
            sd = k * 8 + g * 2 + d
            slot = yd * 8 + g * 2 + d
            for p in range(2):
                self_part = jnp.logical_and(jnp.logical_and(sd == s, yd == y), k == p)
                full_at, packed_at = z_places(s, y, p)
                full = remote(
                    zsend.at[slot, p], zc.at[full_at],
                    ss.at[7], zr_sem.at[s], dev(sd, yd, p),
                )
                packed = remote(
                    zspk.at[slot, :, pl.ds(p * 16, 16), :], zpk.at[packed_at],
                    ss.at[7], zr_sem.at[s], dev(sd, yd, p),
                )

                @pl.when(jnp.logical_not(self_part))
                def _():
                    full.start()
                    packed.start()

                @pl.when(self_part)
                def _():
                    zc[full_at] = zsend[slot, p]
                    zpk[packed_at] = zspk[slot, :, p * 16 : p * 16 + 16, :]

    def z_compute(i, _):
        yd = (y + i * (1 + 2 * k)) % 4
        g = (i // 4 + ZG) % 4
        yr = (i * (1 + 2 * k)) % 4
        values = []
        for t in range(3):
            jl = g * 3 + t
            acc = None
            for slot in range(5):
                c = c2s[yd, k * 12 + jl, slot]
                tile = a2[yr, pl.ds(pl.multiple_of((jl * 5 + slot) * 128, 128), 128), :]
                part = lax.dot_general(xr[c], tile, NT, preferred_element_type=F32)
                acc = part if acc is None else acc + part
            inv = 1.0 / acc[192:193, :]
            values.append(acc[0:192, :] * inv)
        out = yd * 8 + g * 2
        for p in range(2):
            rows = slice(p * 96, p * 96 + 96)
            zsend[out, p] = values[0][rows].astype(BF).reshape(3, 32, 128)
            zsend[out + 1, p] = values[2][rows].astype(BF).reshape(3, 32, 128)
        top, bottom = values[1][0:96], values[1][96:192]
        even = jnp.where(mask96, top, swap(bottom))
        odd = jnp.where(mask96, swap(top), bottom)
        zspk[out] = even.astype(BF).reshape(3, 32, 128)
        zspk[out + 1] = odd.astype(BF).reshape(3, 32, 128)

        @pl.when(i > 0)
        def _():
            z_copies(i - 1)

        return 0

    def z_forward(src_s, p):
        full, packed = pl.ds((src_s * 2 + p) * 3, 3), pl.ds(src_s * 3, 3)
        return [
            remote(ref, ref, ss.at[8], ff_sem.at[src_s], dev(s, y, 1 - k))
            for ref in (zc.at[full, :, pl.ds(0, 128)], zpk.at[p, packed])
        ]

    def z_source(n):
        c = ((s % 8) // 2 + 4 - n // 16) % 4
        r = (n // 4) % 4
        xs = c % 2 + 2 * (r % 2)
        zs = ((c + 4 - xs) // 2) % 2 + 2 * (r // 2)
        return zs * 4 + xs

    def z_receive(i, _):
        src_s = z_source(i * 4)
        own = jnp.logical_and(src_s == s, s // 8 == k)

        @pl.when(own)
        def _():
            rows_of(432, ss.at[7], zr_sem.at[src_s]).wait_recv()

        @pl.when(jnp.logical_not(own))
        def _():
            rows_of(576, ss.at[7], zr_sem.at[src_s]).wait_recv()

        for cp in z_forward(src_s, k):
            cp.start()
        return 0

    def z_finish(i, _):
        rows_of(576, ss.at[8], ff_sem.at[z_source(i * 4)]).wait_recv()
        return 0

    def z_unpack(n, _):
        i = z_source((n // 3) * 4) * 3 + n % 3
        parts = [zpk[p, i].astype(F32).reshape(4, 16, 128) for p in range(2)]
        packed = jnp.concatenate(parts, axis=1).reshape(128, 128)
        lane = lax.broadcasted_iota(jnp.int32, (128, 128), 1)
        fill = jnp.where(lane == 64, 1.0, 0.0).astype(F32)
        block = (i // 3) * 6 + i % 3
        zc[block, :, 128:256] = jnp.where(lane < 64, packed, fill).astype(BF)
        zc[block + 3, :, 128:256] = jnp.where(lane < 64, swap(packed), fill).astype(BF)
        return 0

    def second_stage():
        state_wait()
        lax.fori_loop(0, 16, z_compute, 0)
        z_copies(15)
        for phase in range(5):
            if phase < 4:
                lax.fori_loop(phase * 4, phase * 4 + 4, z_receive, 0)
            if phase > 0:
                lax.fori_loop(phase * 4 - 4, phase * 4, z_finish, 0)
                lax.fori_loop(phase * 12 - 12, phase * 12, z_unpack, 0)

        own = s // 8 == k

        @pl.when(own)
        def _():
            rows_of(32 * 288 - 144, ss.at[7], sr.at[4]).wait_send()

        @pl.when(jnp.logical_not(own))
        def _():
            rows_of(32 * 288, ss.at[7], sr.at[4]).wait_send()

        rows_of(16 * 576, ss.at[8], sr.at[4]).wait_send()

    def partner_at(i, sign):
        j = i // 2
        dz = (j % 4) * (1 + 2 * k) * sign
        xa = (x + 2 * ((j // 4 + j) % 2)) % 4
        return ((z + dz) % 4) * 4 + xa + (i % 2) * (1 - 2 * (xa % 2))

    def target(i):
        return partner_at(i, 1)

    def p_copies(i, last):
        sd = target(i)
        if last:
            full = (pfull.at[pl.ds(sd * 3, 3)], outf.at[s])
            packed = (ppk.at[sd], outp.at[s])
            pair = [
                remote(*full, ss.at[9], sr.at[9], dev(sd, y, k)),
                remote(*packed, ss.at[9], sr.at[9], dev(sd, y, k)),
            ]
            mine = [
                pltpu.make_async_copy(*full, lsem.at[5]),
                pltpu.make_async_copy(*packed, lsem.at[6]),
            ]

            @pl.when(sd != s)
            def _():
                for cp in pair:
                    cp.start()

            @pl.when(sd == s)
            def _():
                for cp in mine:
                    cp.start()

            return
        for step in range(4):
            yd = (y + step) % 4
            pair = [
                remote(
                    pfull.at[pl.ds(sd * 3, 3), pl.ds(pl.multiple_of(yd * 32, 32), 32)], prf.at[me],
                    ss.at[9], qr_sem.at[y * 8 + s // 2], dev(sd, yd, k),
                ),
                remote(
                    ppk.at[sd, yd], prp.at[me],
                    ss.at[9], qr_sem.at[y * 8 + s // 2], dev(sd, yd, k),
                ),
            ]

            if step > 0:
                for cp in pair:
                    cp.start()
                continue

            @pl.when(sd != s)
            def _():
                for cp in pair:
                    cp.start()

            @pl.when(sd == s)
            def _():
                prf[me] = pfull[pl.ds(sd * 3, 3), pl.ds(pl.multiple_of(y * 32, 32), 32), :]
                prp[me] = ppk[sd, y]

    def p_compute(last, i, _):
        sd = target(i)
        for t in range(3):
            acc = None
            for slot in range(5):
                c = c1s[sd, t, slot]
                tile = a1[pl.ds(pl.multiple_of((sd * 15 + t * 5 + slot) * 128, 128), 128), :]
                part = lax.dot_general(
                    tile, zc[c], NN, preferred_element_type=F32
                )
                acc = part if acc is None else acc + part
            inv = 1.0 / acc[:, 192:193]
            first = (acc[:, 0:128] * inv).astype(BF)
            second = (acc[:, 128:256] * inv).astype(BF).astype(F32)
            second = jnp.where(half_lanes((128, 128)), second, 0.0)
            total = first.astype(F32) + second
            mpart[...] += jnp.sum(total.reshape(16, 8, 128), axis=0)
            pfull[sd * 3 + t] = first
            ph[t] = second
        for yd in range(4):
            if last:
                flat = ph[...].reshape(384, 128)
                low = flat[yd * 48 : yd * 48 + 48]
                high = flat[192 + yd * 48 : 240 + yd * 48]
            else:
                low = ph[:, yd * 32 : yd * 32 + 16, :].reshape(48, 128)
                high = ph[:, yd * 32 + 16 : yd * 32 + 32, :].reshape(48, 128)
            ppk[sd, yd] = (low + swap(high)).astype(BF)

        @pl.when(jnp.logical_and(i > 0, i <= HELD))
        def _():
            p_copies(i - 1, last)

        return 0

    def first_stage(last, it):
        mpart[...] = jnp.zeros((8, 128), F32)
        lax.fori_loop(0, 16, functools.partial(p_compute, last), 0)
        mine = jnp.sum(MIX * mpart[...] + (1.0 - MIX) * macc[...], axis=0, keepdims=True)
        mbuf[it, me] = mine
        msend[it] = mine

        def total_copy(i, src, dst):
            return remote(
                msend.at[it], mbuf.at[it, src], ss.at[10], sr.at[10], dev(dst // 4, dst % 4, k)
            )

        def total_send(i, _):
            total_copy(i, me, (me + i) % 64).start()
            return 0

        def late(i, _):
            p_copies(i, last)
            return 0

        lax.fori_loop(1, 64, total_send, 0)
        lax.fori_loop(HELD, 16, late, 0)
        all_of(mbuf.at[it, pl.ds(0, 63)], 10).wait()
        mtot[it, 0] = jnp.sum(mbuf[it], axis=0)
        exchange = remote(
            mtot.at[it, 0], mtot.at[it, 1], ss.at[11], sr.at[11], dev(s, y, 1 - k)
        )
        exchange.start()
        exchange.wait()
        grand = jnp.sum(mtot[it, 0] + mtot[it, 1])
        return jnp.full((8, 128), CELLS / grand, F32)

    def p_wait(group):
        own = group == y * 8 + s // 2

        @pl.when(own)
        def _():
            rows_of(144, ss.at[9], qr_sem.at[group]).wait_recv()

        @pl.when(jnp.logical_not(own))
        def _():
            rows_of(288, ss.at[9], qr_sem.at[group]).wait_recv()

    def update_group(n):
        src_s = partner_at((n // 4) * 2, 3)
        return ((y + 4 - n % 4) % 4) * 8 + src_s // 2

    def update(scale, n, _):
        group = update_group(n)
        ys = group // 8
        even = ((group % 8) * 2) * 4 + ys
        odd = even + 4
        p_wait(group)
        a, b = prp[even].astype(F32), prp[odd].astype(F32)
        mid_top = jnp.where(mask48, a, swap(b))
        mid_bottom = jnp.where(mask48, swap(a), b)
        mid = jnp.concatenate(
            [mid_top.reshape(3, 16, 128), mid_bottom.reshape(3, 16, 128)], axis=1
        ).reshape(96, 128)
        first, third = prf[even].astype(F32), prf[odd].astype(F32)
        for t, value in enumerate((first.reshape(96, 128), mid, third.reshape(96, 128))):
            col = pl.multiple_of((group % 8) * 384 + t * 128, 128)
            before = prior_r[ys, :, :, pl.ds(col, 128)].reshape(96, 128)
            now = (MIX * value + (1.0 - MIX) * before) * scale
            xr[group * 3 + t, pl.ds(pl.multiple_of(k * 96, 16), 96), :] = now.astype(BF)

        @pl.when(n > 0)
        def _():
            forward_state(update_group(n - 1)).start()

        return 0

    second_stage()
    stage5(0)
    rows_of(15 * 1920, ss.at[4], sr.at[4]).wait_send()
    rows_of(15 * 1440, ss.at[5], sr.at[4]).wait_send()
    m1 = first_stage(False, 0)
    scale = m1[0:1, :]
    lax.fori_loop(0, 32, functools.partial(update, scale), 0)
    forward_state(update_group(31)).start()

    rows_of(63 * 144, ss.at[9], sr.at[4]).wait_send()

    second_stage()
    mout[...] = first_stage(True, 1)

    rows_of(15 * 576, ss.at[9], sr.at[9]).wait()
    pltpu.make_async_copy(pfull.at[pl.ds(s * 3, 3)], outf.at[s], lsem.at[5]).wait()
    pltpu.make_async_copy(ppk.at[s], outp.at[s], lsem.at[6]).wait()


def run_main(prior, t1, t2, c1, c2):
    any_spec = pl.BlockSpec(memory_space=pl.ANY)
    vmem = pl.BlockSpec(memory_space=pltpu.VMEM)
    dma = pltpu.SemaphoreType.DMA
    scratch = [
        pltpu.VMEM((4, 3, 32, 3072), F32),
        pltpu.VMEM((30720, 128), BF),
        pltpu.VMEM((4, 7680, 128), BF),
        pltpu.VMEM((96, 208, 128), BF),
        pltpu.VMEM((96, 128, 256), BF),
        pltpu.VMEM((2, 48, 64, 128), BF),
        pltpu.VMEM((32, 2, 3, 32, 128), BF),
        pltpu.VMEM((32, 3, 32, 128), BF),
        pltpu.VMEM((48, 128, 128), BF),
        pltpu.VMEM((16, 4, 48, 128), BF),
        pltpu.VMEM((3, 128, 128), F32),
        pltpu.VMEM((64, 3, 32, 128), BF),
        pltpu.VMEM((64, 48, 128), BF),
        pltpu.VMEM((2, 64, 1, 128), F32),
        pltpu.VMEM((2, 1, 128), F32),
        pltpu.VMEM((8, 128), F32),
        pltpu.VMEM((2, 2, 1, 128), F32),
        pltpu.VMEM((8, 128), F32),
        pltpu.VMEM((8, 128), jnp.int32),
        pltpu.VMEM((24, 128), jnp.int32),
        pltpu.VMEM((16, 8, 128), jnp.int32),
        pltpu.VMEM((4, 24, 128), jnp.int32),
        pltpu.SMEM((16, 8, 128), jnp.int32),
        pltpu.SMEM((4, 24, 128), jnp.int32),
        pltpu.SemaphoreType.REGULAR((3,)),
        dma((7,)), dma((12,)), dma((12,)), dma((2, 2, 5, 4)), dma((16,)), dma((16,)), dma((32,)),
    ]
    return pl.pallas_call(
        main_kernel,
        out_shape=(
            jax.ShapeDtypeStruct((16, 3, 128, 128), BF),
            jax.ShapeDtypeStruct((16, 4, 48, 128), BF),
            jax.ShapeDtypeStruct((8, 128), F32),
        ),
        in_specs=[any_spec, any_spec, any_spec, vmem, vmem],
        out_specs=(any_spec, any_spec, vmem),
        scratch_shapes=scratch,
        compiler_params=pltpu.CompilerParams(
            collective_id=0, has_side_effects=True, vmem_limit_bytes=60 << 20
        ),
        name="align",
    )(prior, t1, t2, c1, c2)


def combine_kernel(pf, pp, m, prior, out):
    mask = half_lanes((192, 128))
    scale = m[0:1, :]
    for q in range(CQ):
        cols = pl.ds(q * 384, 384)
        pair = pl.ds(q * 2, 2)
        combine_pair(pf.at[pair], pp.at[pair], scale, mask, prior.at[:, cols], out.at[:, cols])


def combine_pair(pf, pp, scale, mask, prior, out):
    a, b = pp[0].astype(F32), pp[1].astype(F32)
    mid = jnp.concatenate([jnp.where(mask, a, swap(b)), jnp.where(mask, swap(a), b)], axis=0)
    for t, value in enumerate((pf[0].astype(F32), mid, pf[1].astype(F32))):
        cols = slice(t * 128, (t + 1) * 128)
        out[:, cols] = (MIX * value + (1.0 - MIX) * prior[:, cols]) * scale


def combine(pf, pp, m, prior):
    return pl.pallas_call(
        combine_kernel,
        grid=(8 // CQ,),
        out_shape=jax.ShapeDtypeStruct((384, 3072), F32),
        in_specs=[
            pl.BlockSpec((2 * CQ, 384, 128), lambda i: (i, 0, 0)),
            pl.BlockSpec((2 * CQ, 192, 128), lambda i: (i, 0, 0)),
            pl.BlockSpec((8, 128), lambda i: (0, 0)),
            pl.BlockSpec((384, 384 * CQ), lambda i: (0, i)),
        ],
        out_specs=pl.BlockSpec((384, 384 * CQ), lambda i: (0, i)),
        name="combine",
    )(pf, pp, m, prior)


def local(prior_scores, tiles_first, columns_first, tiles_second, columns_second):
    t1 = tiles_first.reshape(1920, 128)
    t2 = tiles_second.reshape(15360, 128)
    pf, pp, m = run_main(
        prior_scores.reshape(3, 128, 3072), t1, t2, columns_first, columns_second
    )
    return combine(
        pf.reshape(16, 384, 128), pp.reshape(16, 192, 128), m, prior_scores
    )


def solution(mesh):
    return jax.shard_map(
        local,
        mesh=mesh,
        in_specs=(
            P("row", "col"),
            P("row", None, None, None),
            P("row", None),
            P("col", None, None, None),
            P("col", None),
        ),
        out_specs=P("row", "col"),
        check_vma=False,
    )
```

```python
import functools

import jax
import jax.numpy as jnp
from jax import lax
from jax.experimental import pallas as pl
from jax.experimental.pallas import tpu as pltpu
from jax.sharding import PartitionSpec as P

MESH = pl.DeviceIdType.MESH
BF = jnp.bfloat16
F32 = jnp.float32
MIX = 0.8
CELLS = float(12288 * 12288)
HELD = 8
CQ = 4
NT = (((1,), (1,)), ((), ()))
NN = (((1,), (0,)), ((), ()))


def half_lanes(shape):
    return lax.broadcasted_iota(jnp.int32, shape, 1) < 64


def swap(value):
    return pltpu.roll(value, 64, 1)


def main_kernel(
    prior, t1, t2, c1, c2,
    outf, outp, mout,
    prior_r, a1, a2, xr, zc, zpk, zsend, zspk, pfull, ppk, ph, prf, prp,
    mbuf, msend, mpart, mtot, macc, c1p, c2p, c1g, c2g, c1s, c2s,
    rounds, lsem, ss, sr, gr_sem, zr_sem, ff_sem, qr_sem,
):
    row = lax.axis_index("row")
    y = lax.axis_index("col")
    k = row % 2
    s = row // 2
    x = s % 4
    z = s // 4
    me = s * 4 + y

    def dev(s_, y_, k_):
        return {"row": s_ * 2 + k_, "col": y_}

    def remote(src, dst, ssem, rsem, target):
        return pltpu.make_async_remote_copy(
            src_ref=src, dst_ref=dst, send_sem=ssem, recv_sem=rsem,
            device_id=target, device_id_type=MESH,
        )

    def all_of(ref, number):
        return remote(ref, ref, ss.at[number], sr.at[number], dev(s, y, 1 - k))

    def rows_of(count, send, recv):
        ref = a1.at[pl.ds(0, count)]
        return remote(ref, ref, send, recv, dev(s, y, 1 - k))

    x_line = [dev(z * 4 + (x + d) % 4, y, k) for d in (1, 2, 3)]
    z_line = [dev(((z + d) % 4) * 4 + x, y, k) for d in (1, 2, 3)]
    y_line = [dev(s, (y + d) % 4, k) for d in (1, 2, 3)]
    pair_line = [dev(s, y, 1 - k)]

    def greet(sem, peers):
        for peer in peers:
            pl.semaphore_signal(sem, inc=1, device_id=peer, device_id_type=MESH)

    barrier = pltpu.get_barrier_semaphore()
    greet(barrier, x_line + z_line + y_line + pair_line)

    load1 = pltpu.make_async_copy(t1, a1.at[pl.ds(s * 1920, 1920)], lsem.at[0])
    load1.start()
    load2 = pltpu.make_async_copy(t2.at[pl.ds(k * 7680, 7680)], a2.at[0], lsem.at[1])
    load2.start()
    load3 = pltpu.make_async_copy(
        prior.at[:, pl.ds(pl.multiple_of(y * 32, 32), 32), :], prior_r.at[y], lsem.at[2]
    )
    load3.start()
    c1p[0:3, 0:5] = c1[...]
    c2p[:, 0:5] = c2[...]
    c1g[s] = c1p[...]
    c2g[y] = c2p[...]
    xr[:, 192:208, :] = jnp.ones((96, 16, 128), BF)
    pl.semaphore_wait(barrier, 10)
    greet(rounds.at[0], x_line)

    for d in (1, 3, 2):
        yd = (y + d) % 4
        cp = remote(
            t2.at[pl.ds(k * 7680 + s * 480, 480)],
            a2.at[(4 - d) % 4, pl.ds(s * 480, 480)],
            ss.at[2], sr.at[2], dev(s, yd, k),
        )
        cp.start()
        cc = remote(c2p, c2g.at[y], ss.at[1], sr.at[1], dev(s, yd, k))
        cc.start()

    XP, XM = (z * 4 + (x + 1) % 4), (z * 4 + (x + 3) % 4)
    ZP, ZM = (((z + 1) % 4) * 4 + x), (((z + 3) % 4) * 4 + x)

    def region(kind, origin, part):
        if kind == 0:
            off, size = ((0, 480), (480, 480), (960, 480), (1440, 480), (0, 960), (960, 960))[part]
            return a1.at[pl.ds(pl.multiple_of(origin * 1920 + off, 16), size)]
        off, size = ((0, 128), (128, 112), (240, 128), (368, 112), (0, 240), (240, 240))[part]
        return a2.at[pl.ds(1, 3), pl.ds(pl.multiple_of(origin * 480 + off, 16), size)]

    def nbr(axis, up):
        return (XP if up else XM) if axis == 0 else (ZP if up else ZM)

    def shifted(axis, origin, delta):
        ox, oz = origin % 4, origin // 4
        if axis == 0:
            return oz * 4 + (ox + delta) % 4
        return ((oz + delta) % 4) * 4 + ox

    def hop(kind, half, group, slot, origin, part, axis, up):
        cp = remote(
            region(kind, origin, part), region(kind, origin, part),
            ss.at[4 + kind], gr_sem.at[kind, half, group, slot],
            dev(nbr(axis, up), y, k),
        )
        cp.start()

    def landed(kind, half, group, slot, origin, part):
        cp = remote(
            region(kind, origin, part), region(kind, origin, part),
            ss.at[4 + kind], gr_sem.at[kind, half, group, slot],
            dev(nbr(0, True), y, k),
        )
        cp.wait_recv()

    def whole(half):
        return 4 + half

    def ring_start(kind, half, group, origin, axis):
        hop(kind, half, group, 0, origin, whole(half), axis, True)
        hop(kind, half, group, 1, origin, whole(half), axis, False)

    def ring_relay(kind, half, group, base, axis):
        low, high = shifted(axis, base, 3), shifted(axis, base, 1)
        landed(kind, half, group, 0, low, whole(half))
        hop(kind, half, group, 2, low, 2 * half, axis, True)
        landed(kind, half, group, 1, high, whole(half))
        hop(kind, half, group, 3, high, 2 * half + 1, axis, False)

    def ring_end(kind, half, group, base, axis):
        far = shifted(axis, base, 2)
        landed(kind, half, group, 2, far, 2 * half)
        landed(kind, half, group, 3, far, 2 * half + 1)

    def stage1(kind):
        for half in (0, 1):
            ring_start(kind, half, 0, s, half)
        for half in (0, 1):
            ring_start(kind, half, 1, s, 1 - half)

    def stage2(kind):
        for half in (0, 1):
            ring_relay(kind, half, 0, s, half)
            for g, delta in ((2, 3), (3, 1)):
                ring_start(kind, half, g, shifted(half, s, delta), 1 - half)

    def stage3(kind):
        for half in (0, 1):
            ring_end(kind, half, 0, s, half)
            ring_start(kind, half, 4, shifted(half, s, 2), 1 - half)

    def stage4(kind):
        for g, delta in ((1, 0), (2, 3), (3, 1), (4, 2)):
            for half in (0, 1):
                ring_relay(kind, half, g, shifted(half, s, delta), 1 - half)

    def stage5(kind):
        for g, delta in ((1, 0), (2, 3), (3, 1), (4, 2)):
            for half in (0, 1):
                ring_end(kind, half, g, shifted(half, s, delta), 1 - half)

    load1.wait()
    stage1(0)
    for d in (1, 3, 2):
        yd = (y + d) % 4
        cp = remote(
            prior.at[:, pl.ds(pl.multiple_of(yd * 32, 32), 32), :], prior_r.at[y],
            ss.at[3], sr.at[3], dev(s, yd, k),
        )
        cp.start()

    def send_columns(i, _):
        remote(
            c1p, c1g.at[s], ss.at[0], sr.at[0], dev((s + i) % 16, y, k)
        ).start()
        return 0

    pl.semaphore_wait(rounds.at[0], 3)
    greet(rounds.at[1], z_line)
    lax.fori_loop(1, 16, send_columns, 0)

    all_of(a2.at[pl.ds(1, 3), pl.ds(0, 480)], 2).wait()
    stage1(1)
    stage2(1)
    stage2(0)
    stage3(1)
    stage3(0)
    load3.wait()
    load2.wait()

    pl.semaphore_wait(rounds.at[1], 3)
    greet(rounds.at[2], pair_line)

    all_of(c2g.at[pl.ds(0, 3)], 1).wait()
    all_of(c1g.at[pl.ds(0, 15)], 0).wait()
    cps = [
        pltpu.make_async_copy(c1g, c1s, lsem.at[3]),
        pltpu.make_async_copy(c2g, c2s, lsem.at[4]),
    ]
    for cp in cps:
        cp.start()
    for cp in cps:
        cp.wait()

    stage4(1)
    pl.semaphore_wait(rounds.at[2], 1)
    stage4(0)
    all_of(prior_r.at[pl.ds(0, 3)], 3).wait()

    mask96 = half_lanes((96, 128))
    mask48 = half_lanes((48, 128))

    def forward_state(group):
        return remote(
            xr.at[pl.ds(group * 3, 3), pl.ds(k * 96, 96)],
            xr.at[pl.ds(group * 3, 3), pl.ds(k * 96, 96)],
            ss.at[6], sr.at[6], dev(s, y, 1 - k),
        )

    def state_wait():
        all_of(xr.at[:, pl.ds(pl.multiple_of((1 - k) * 96, 16), 96)], 6).wait()

    macc[...] = jnp.zeros((8, 128), F32)

    def convert(group, _):
        ys = group // 8
        for t in range(3):
            col = pl.multiple_of((group % 8) * 384 + t * 128, 128)
            value = prior_r[ys, :, :, pl.ds(col, 128)].reshape(96, 128)
            macc[...] += jnp.sum(value.reshape(12, 8, 128), axis=0)
            xr[group * 3 + t, pl.ds(pl.multiple_of(k * 96, 16), 96), :] = value.astype(BF)

        @pl.when(group > 0)
        def _():
            forward_state(group - 1).start()

        return 0

    lax.fori_loop(0, 32, convert, 0)
    forward_state(31).start()
    stage5(1)

    def z_places(src_s, src_y, p):
        return (
            (
                pl.ds((src_s * 2 + p) * 3, 3),
                pl.ds(pl.multiple_of(src_y * 32, 32), 32),
                pl.ds(0, 128),
            ),
            (
                p,
                pl.ds(src_s * 3, 3),
                pl.ds(pl.multiple_of(src_y * 16, 16), 16),
                pl.ds(0, 128),
            ),
        )

    ZG = x + 2 * z

    def z_copies(i):
        yd = (y + i * (1 + 2 * k)) % 4
        g = (i // 4 + ZG) % 4
        for d in range(2):
            sd = k * 8 + g * 2 + d
            slot = yd * 8 + g * 2 + d
            for p in range(2):
                self_part = jnp.logical_and(jnp.logical_and(sd == s, yd == y), k == p)
                full_at, packed_at = z_places(s, y, p)
                full = remote(
                    zsend.at[slot, p], zc.at[full_at],
                    ss.at[7], zr_sem.at[s], dev(sd, yd, p),
                )
                packed = remote(
                    zspk.at[slot, :, pl.ds(p * 16, 16), :], zpk.at[packed_at],
                    ss.at[7], zr_sem.at[s], dev(sd, yd, p),
                )

                @pl.when(jnp.logical_not(self_part))
                def _():
                    full.start()
                    packed.start()

                @pl.when(self_part)
                def _():
                    zc[full_at] = zsend[slot, p]
                    zpk[packed_at] = zspk[slot, :, p * 16 : p * 16 + 16, :]

    def z_compute(i, _):
        yd = (y + i * (1 + 2 * k)) % 4
        g = (i // 4 + ZG) % 4
        yr = (i * (1 + 2 * k)) % 4
        values = []
        for t in range(3):
            jl = g * 3 + t
            acc = None
            for slot in range(5):
                c = c2s[yd, k * 12 + jl, slot]
                tile = a2[yr, pl.ds(pl.multiple_of((jl * 5 + slot) * 128, 128), 128), :]
                part = lax.dot_general(xr[c], tile, NT, preferred_element_type=F32)
                acc = part if acc is None else acc + part
            inv = 1.0 / acc[192:193, :]
            values.append(acc[0:192, :] * inv)
        out = yd * 8 + g * 2
        for p in range(2):
            rows = slice(p * 96, p * 96 + 96)
            zsend[out, p] = values[0][rows].astype(BF).reshape(3, 32, 128)
            zsend[out + 1, p] = values[2][rows].astype(BF).reshape(3, 32, 128)
        top, bottom = values[1][0:96], values[1][96:192]
        even = jnp.where(mask96, top, swap(bottom))
        odd = jnp.where(mask96, swap(top), bottom)
        zspk[out] = even.astype(BF).reshape(3, 32, 128)
        zspk[out + 1] = odd.astype(BF).reshape(3, 32, 128)

        @pl.when(i > 0)
        def _():
            z_copies(i - 1)

        return 0

    def z_forward(src_s, p):
        full, packed = pl.ds((src_s * 2 + p) * 3, 3), pl.ds(src_s * 3, 3)
        return [
            remote(ref, ref, ss.at[8], ff_sem.at[src_s], dev(s, y, 1 - k))
            for ref in (zc.at[full, :, pl.ds(0, 128)], zpk.at[p, packed])
        ]

    def z_source(n):
        c = ((s % 8) // 2 + 4 - n // 16) % 4
        r = (n // 4) % 4
        xs = c % 2 + 2 * (r % 2)
        zs = ((c + 4 - xs) // 2) % 2 + 2 * (r // 2)
        return zs * 4 + xs

    def z_receive(i, _):
        src_s = z_source(i * 4)
        own = jnp.logical_and(src_s == s, s // 8 == k)

        @pl.when(own)
        def _():
            rows_of(432, ss.at[7], zr_sem.at[src_s]).wait_recv()

        @pl.when(jnp.logical_not(own))
        def _():
            rows_of(576, ss.at[7], zr_sem.at[src_s]).wait_recv()

        for cp in z_forward(src_s, k):
            cp.start()
        return 0

    def z_finish(i, _):
        rows_of(576, ss.at[8], ff_sem.at[z_source(i * 4)]).wait_recv()
        return 0

    def z_unpack(n, _):
        i = z_source((n // 3) * 4) * 3 + n % 3
        parts = [zpk[p, i].astype(F32).reshape(4, 16, 128) for p in range(2)]
        packed = jnp.concatenate(parts, axis=1).reshape(128, 128)
        lane = lax.broadcasted_iota(jnp.int32, (128, 128), 1)
        fill = jnp.where(lane == 64, 1.0, 0.0).astype(F32)
        block = (i // 3) * 6 + i % 3
        zc[block, :, 128:256] = jnp.where(lane < 64, packed, fill).astype(BF)
        zc[block + 3, :, 128:256] = jnp.where(lane < 64, swap(packed), fill).astype(BF)
        return 0

    def z_complete(i, _):
        z_finish(i, 0)
        for t in range(3):
            z_unpack(i * 3 + t, 0)
        return 0

    def second_stage():
        state_wait()
        lax.fori_loop(0, 16, z_compute, 0)
        z_copies(15)
        for phase in range(5):
            if phase < 4:
                lax.fori_loop(phase * 4, phase * 4 + 4, z_receive, 0)
            if phase > 0:
                lax.fori_loop(phase * 4 - 4, phase * 4, z_complete, 0)

        own = s // 8 == k

        @pl.when(own)
        def _():
            rows_of(32 * 288 - 144, ss.at[7], sr.at[4]).wait_send()

        @pl.when(jnp.logical_not(own))
        def _():
            rows_of(32 * 288, ss.at[7], sr.at[4]).wait_send()

        rows_of(16 * 576, ss.at[8], sr.at[4]).wait_send()

    def partner_at(i, sign):
        j = i // 2
        dz = ((j + 1) % 4) * (1 + 2 * k) * sign
        xa = (x + 2 * ((j // 4 + j) % 2)) % 4
        return ((z + dz) % 4) * 4 + xa + (i % 2) * (1 - 2 * (xa % 2))

    def target(i):
        return partner_at(i, 1)

    def p_copies(i, last):
        sd = target(i)
        if last:
            full = (pfull.at[pl.ds(sd * 3, 3)], outf.at[s])
            packed = (ppk.at[sd], outp.at[s])
            pair = [
                remote(*full, ss.at[9], sr.at[9], dev(sd, y, k)),
                remote(*packed, ss.at[9], sr.at[9], dev(sd, y, k)),
            ]
            mine = [
                pltpu.make_async_copy(*full, lsem.at[5]),
                pltpu.make_async_copy(*packed, lsem.at[6]),
            ]

            @pl.when(sd != s)
            def _():
                for cp in pair:
                    cp.start()

            @pl.when(sd == s)
            def _():
                for cp in mine:
                    cp.start()

            return
        for step in range(4):
            yd = (y + step) % 4
            pair = [
                remote(
                    pfull.at[pl.ds(sd * 3, 3), pl.ds(pl.multiple_of(yd * 32, 32), 32)], prf.at[me],
                    ss.at[9], qr_sem.at[y * 8 + s // 2], dev(sd, yd, k),
                ),
                remote(
                    ppk.at[sd, yd], prp.at[me],
                    ss.at[9], qr_sem.at[y * 8 + s // 2], dev(sd, yd, k),
                ),
            ]

            if step > 0:
                for cp in pair:
                    cp.start()
                continue

            @pl.when(sd != s)
            def _():
                for cp in pair:
                    cp.start()

            @pl.when(sd == s)
            def _():
                prf[me] = pfull[pl.ds(sd * 3, 3), pl.ds(pl.multiple_of(y * 32, 32), 32), :]
                prp[me] = ppk[sd, y]

    def p_compute(last, i, _):
        sd = target(i)
        for t in range(3):
            acc = None
            for slot in range(5):
                c = c1s[sd, t, slot]
                tile = a1[pl.ds(pl.multiple_of((sd * 15 + t * 5 + slot) * 128, 128), 128), :]
                part = lax.dot_general(
                    tile, zc[c], NN, preferred_element_type=F32
                )
                acc = part if acc is None else acc + part
            inv = 1.0 / acc[:, 192:193]
            first = (acc[:, 0:128] * inv).astype(BF)
            second = (acc[:, 128:256] * inv).astype(BF).astype(F32)
            second = jnp.where(half_lanes((128, 128)), second, 0.0)
            total = first.astype(F32) + second
            mpart[...] += jnp.sum(total.reshape(16, 8, 128), axis=0)
            pfull[sd * 3 + t] = first
            ph[t] = second
        for yd in range(4):
            if last:
                flat = ph[...].reshape(384, 128)
                low = flat[yd * 48 : yd * 48 + 48]
                high = flat[192 + yd * 48 : 240 + yd * 48]
            else:
                low = ph[:, yd * 32 : yd * 32 + 16, :].reshape(48, 128)
                high = ph[:, yd * 32 + 16 : yd * 32 + 32, :].reshape(48, 128)
            ppk[sd, yd] = (low + swap(high)).astype(BF)

        @pl.when(jnp.logical_and(i > 0, i <= HELD))
        def _():
            p_copies(i - 1, last)

        return 0

    def first_stage(last, it):
        mpart[...] = jnp.zeros((8, 128), F32)
        lax.fori_loop(0, 16, functools.partial(p_compute, last), 0)
        mine = jnp.sum(MIX * mpart[...] + (1.0 - MIX) * macc[...], axis=0, keepdims=True)
        mbuf[it, me] = mine
        msend[it] = mine

        def total_copy(i, src, dst):
            return remote(
                msend.at[it], mbuf.at[it, src], ss.at[10], sr.at[10], dev(dst // 4, dst % 4, k)
            )

        def total_send(i, _):
            total_copy(i, me, (me + i) % 64).start()
            return 0

        def late(i, _):
            p_copies(i, last)
            return 0

        lax.fori_loop(1, 64, total_send, 0)
        lax.fori_loop(HELD, 16, late, 0)
        all_of(mbuf.at[it, pl.ds(0, 63)], 10).wait()
        mtot[it, 0] = jnp.sum(mbuf[it], axis=0)
        exchange = remote(
            mtot.at[it, 0], mtot.at[it, 1], ss.at[11], sr.at[11], dev(s, y, 1 - k)
        )
        exchange.start()
        exchange.wait()
        grand = jnp.sum(mtot[it, 0] + mtot[it, 1])
        return jnp.full((8, 128), CELLS / grand, F32)

    def p_wait(group):
        own = group == y * 8 + s // 2

        @pl.when(own)
        def _():
            rows_of(144, ss.at[9], qr_sem.at[group]).wait_recv()

        @pl.when(jnp.logical_not(own))
        def _():
            rows_of(288, ss.at[9], qr_sem.at[group]).wait_recv()

    def update_group(n):
        src_s = partner_at((n // 4) * 2, 3)
        return ((y + 4 - n % 4) % 4) * 8 + src_s // 2

    def update(scale, n, _):
        group = update_group(n)
        ys = group // 8
        even = ((group % 8) * 2) * 4 + ys
        odd = even + 4
        p_wait(group)
        a, b = prp[even].astype(F32), prp[odd].astype(F32)
        mid_top = jnp.where(mask48, a, swap(b))
        mid_bottom = jnp.where(mask48, swap(a), b)
        mid = jnp.concatenate(
            [mid_top.reshape(3, 16, 128), mid_bottom.reshape(3, 16, 128)], axis=1
        ).reshape(96, 128)
        first, third = prf[even].astype(F32), prf[odd].astype(F32)
        for t, value in enumerate((first.reshape(96, 128), mid, third.reshape(96, 128))):
            col = pl.multiple_of((group % 8) * 384 + t * 128, 128)
            before = prior_r[ys, :, :, pl.ds(col, 128)].reshape(96, 128)
            now = (MIX * value + (1.0 - MIX) * before) * scale
            xr[group * 3 + t, pl.ds(pl.multiple_of(k * 96, 16), 96), :] = now.astype(BF)

        @pl.when(n > 0)
        def _():
            forward_state(update_group(n - 1)).start()

        return 0

    second_stage()
    stage5(0)
    rows_of(15 * 1920, ss.at[4], sr.at[4]).wait_send()
    rows_of(15 * 1440, ss.at[5], sr.at[4]).wait_send()
    m1 = first_stage(False, 0)
    scale = m1[0:1, :]
    lax.fori_loop(0, 32, functools.partial(update, scale), 0)
    forward_state(update_group(31)).start()

    rows_of(63 * 144, ss.at[9], sr.at[4]).wait_send()

    second_stage()
    mout[...] = first_stage(True, 1)

    rows_of(15 * 576, ss.at[9], sr.at[9]).wait()
    pltpu.make_async_copy(pfull.at[pl.ds(s * 3, 3)], outf.at[s], lsem.at[5]).wait()
    pltpu.make_async_copy(ppk.at[s], outp.at[s], lsem.at[6]).wait()


def run_main(prior, t1, t2, c1, c2):
    any_spec = pl.BlockSpec(memory_space=pl.ANY)
    vmem = pl.BlockSpec(memory_space=pltpu.VMEM)
    dma = pltpu.SemaphoreType.DMA
    scratch = [
        pltpu.VMEM((4, 3, 32, 3072), F32),
        pltpu.VMEM((30720, 128), BF),
        pltpu.VMEM((4, 7680, 128), BF),
        pltpu.VMEM((96, 208, 128), BF),
        pltpu.VMEM((96, 128, 256), BF),
        pltpu.VMEM((2, 48, 64, 128), BF),
        pltpu.VMEM((32, 2, 3, 32, 128), BF),
        pltpu.VMEM((32, 3, 32, 128), BF),
        pltpu.VMEM((48, 128, 128), BF),
        pltpu.VMEM((16, 4, 48, 128), BF),
        pltpu.VMEM((3, 128, 128), F32),
        pltpu.VMEM((64, 3, 32, 128), BF),
        pltpu.VMEM((64, 48, 128), BF),
        pltpu.VMEM((2, 64, 1, 128), F32),
        pltpu.VMEM((2, 1, 128), F32),
        pltpu.VMEM((8, 128), F32),
        pltpu.VMEM((2, 2, 1, 128), F32),
        pltpu.VMEM((8, 128), F32),
        pltpu.VMEM((8, 128), jnp.int32),
        pltpu.VMEM((24, 128), jnp.int32),
        pltpu.VMEM((16, 8, 128), jnp.int32),
        pltpu.VMEM((4, 24, 128), jnp.int32),
        pltpu.SMEM((16, 8, 128), jnp.int32),
        pltpu.SMEM((4, 24, 128), jnp.int32),
        pltpu.SemaphoreType.REGULAR((3,)),
        dma((7,)), dma((12,)), dma((12,)), dma((2, 2, 5, 4)), dma((16,)), dma((16,)), dma((32,)),
    ]
    return pl.pallas_call(
        main_kernel,
        out_shape=(
            jax.ShapeDtypeStruct((16, 3, 128, 128), BF),
            jax.ShapeDtypeStruct((16, 4, 48, 128), BF),
            jax.ShapeDtypeStruct((8, 128), F32),
        ),
        in_specs=[any_spec, any_spec, any_spec, vmem, vmem],
        out_specs=(any_spec, any_spec, vmem),
        scratch_shapes=scratch,
        compiler_params=pltpu.CompilerParams(
            collective_id=0, has_side_effects=True, vmem_limit_bytes=60 << 20
        ),
        name="align",
    )(prior, t1, t2, c1, c2)


def combine_kernel(pf, pp, m, prior, out):
    mask = half_lanes((192, 128))
    scale = m[0:1, :]
    for q in range(CQ):
        cols = pl.ds(q * 384, 384)
        pair = pl.ds(q * 2, 2)
        combine_pair(pf.at[pair], pp.at[pair], scale, mask, prior.at[:, cols], out.at[:, cols])


def combine_pair(pf, pp, scale, mask, prior, out):
    a, b = pp[0].astype(F32), pp[1].astype(F32)
    mid = jnp.concatenate([jnp.where(mask, a, swap(b)), jnp.where(mask, swap(a), b)], axis=0)
    for t, value in enumerate((pf[0].astype(F32), mid, pf[1].astype(F32))):
        cols = slice(t * 128, (t + 1) * 128)
        out[:, cols] = (MIX * value + (1.0 - MIX) * prior[:, cols]) * scale


def combine(pf, pp, m, prior):
    return pl.pallas_call(
        combine_kernel,
        grid=(8 // CQ,),
        out_shape=jax.ShapeDtypeStruct((384, 3072), F32),
        in_specs=[
            pl.BlockSpec((2 * CQ, 384, 128), lambda i: (i, 0, 0)),
            pl.BlockSpec((2 * CQ, 192, 128), lambda i: (i, 0, 0)),
            pl.BlockSpec((8, 128), lambda i: (0, 0)),
            pl.BlockSpec((384, 384 * CQ), lambda i: (0, i)),
        ],
        out_specs=pl.BlockSpec((384, 384 * CQ), lambda i: (0, i)),
        name="combine",
    )(pf, pp, m, prior)


def local(prior_scores, tiles_first, columns_first, tiles_second, columns_second):
    t1 = tiles_first.reshape(1920, 128)
    t2 = tiles_second.reshape(15360, 128)
    pf, pp, m = run_main(
        prior_scores.reshape(3, 128, 3072), t1, t2, columns_first, columns_second
    )
    return combine(
        pf.reshape(16, 384, 128), pp.reshape(16, 192, 128), m, prior_scores
    )


def solution(mesh):
    return jax.shard_map(
        local,
        mesh=mesh,
        in_specs=(
            P("row", "col"),
            P("row", None, None, None),
            P("row", None),
            P("col", None, None, None),
            P("col", None),
        ),
        out_specs=P("row", "col"),
        check_vma=False,
    )
```

```python
import functools

import jax
import jax.numpy as jnp
from jax import lax
from jax.experimental import pallas as pl
from jax.experimental.pallas import tpu as pltpu
from jax.sharding import PartitionSpec as P

MESH = pl.DeviceIdType.MESH
BF = jnp.bfloat16
F32 = jnp.float32
MIX = 0.8
CELLS = float(12288 * 12288)
HELD = 8
CQ = 4
NT = (((1,), (1,)), ((), ()))
NN = (((1,), (0,)), ((), ()))


def half_lanes(shape):
    return lax.broadcasted_iota(jnp.int32, shape, 1) < 64


def swap(value):
    return pltpu.roll(value, 64, 1)


def main_kernel(
    prior, t1, t2, c1, c2,
    outf, outp, mout,
    prior_r, a1, a2, xr, zc, zpk, zsend, zspk, pfull, ppk, ph, prf, prp,
    mbuf, msend, mpart, mtot, macc, c1p, c2p, c1g, c2g, c1s, c2s,
    rounds, lsem, ss, sr, gr_sem, zr_sem, ff_sem, qr_sem,
):
    row = lax.axis_index("row")
    y = lax.axis_index("col")
    k = row % 2
    s = row // 2
    x = s % 4
    z = s // 4
    me = s * 4 + y

    def dev(s_, y_, k_):
        return {"row": s_ * 2 + k_, "col": y_}

    def remote(src, dst, ssem, rsem, target):
        return pltpu.make_async_remote_copy(
            src_ref=src, dst_ref=dst, send_sem=ssem, recv_sem=rsem,
            device_id=target, device_id_type=MESH,
        )

    def all_of(ref, number):
        return remote(ref, ref, ss.at[number], sr.at[number], dev(s, y, 1 - k))

    def rows_of(count, send, recv):
        ref = a1.at[pl.ds(0, count)]
        return remote(ref, ref, send, recv, dev(s, y, 1 - k))

    x_line = [dev(z * 4 + (x + d) % 4, y, k) for d in (1, 2, 3)]
    z_line = [dev(((z + d) % 4) * 4 + x, y, k) for d in (1, 2, 3)]
    y_line = [dev(s, (y + d) % 4, k) for d in (1, 2, 3)]
    pair_line = [dev(s, y, 1 - k)]

    def greet(sem, peers):
        for peer in peers:
            pl.semaphore_signal(sem, inc=1, device_id=peer, device_id_type=MESH)

    barrier = pltpu.get_barrier_semaphore()
    greet(barrier, x_line + z_line + y_line + pair_line)

    load1 = pltpu.make_async_copy(t1, a1.at[pl.ds(s * 1920, 1920)], lsem.at[0])
    load1.start()
    load2 = pltpu.make_async_copy(t2.at[pl.ds(k * 7680, 7680)], a2.at[0], lsem.at[1])
    load2.start()
    load3 = pltpu.make_async_copy(
        prior.at[:, pl.ds(pl.multiple_of(y * 32, 32), 32), :], prior_r.at[y], lsem.at[2]
    )
    load3.start()
    c1p[0:3, 0:5] = c1[...]
    c2p[:, 0:5] = c2[...]
    c1g[s] = c1p[...]
    c2g[y] = c2p[...]
    xr[:, 192:208, :] = jnp.ones((96, 16, 128), BF)
    pl.semaphore_wait(barrier, 10)
    greet(rounds.at[0], x_line)

    for d in (1, 3, 2):
        yd = (y + d) % 4
        cp = remote(
            t2.at[pl.ds(k * 7680 + s * 480, 480)],
            a2.at[(4 - d) % 4, pl.ds(s * 480, 480)],
            ss.at[2], sr.at[2], dev(s, yd, k),
        )
        cp.start()
        cc = remote(c2p, c2g.at[y], ss.at[1], sr.at[1], dev(s, yd, k))
        cc.start()

    XP, XM = (z * 4 + (x + 1) % 4), (z * 4 + (x + 3) % 4)
    ZP, ZM = (((z + 1) % 4) * 4 + x), (((z + 3) % 4) * 4 + x)

    def region(kind, origin, part):
        if kind == 0:
            off, size = ((0, 480), (480, 480), (960, 480), (1440, 480), (0, 960), (960, 960))[part]
            return a1.at[pl.ds(pl.multiple_of(origin * 1920 + off, 16), size)]
        off, size = ((0, 128), (128, 112), (240, 128), (368, 112), (0, 240), (240, 240))[part]
        return a2.at[pl.ds(1, 3), pl.ds(pl.multiple_of(origin * 480 + off, 16), size)]

    def nbr(axis, up):
        return (XP if up else XM) if axis == 0 else (ZP if up else ZM)

    def shifted(axis, origin, delta):
        ox, oz = origin % 4, origin // 4
        if axis == 0:
            return oz * 4 + (ox + delta) % 4
        return ((oz + delta) % 4) * 4 + ox

    def hop(kind, half, group, slot, origin, part, axis, up):
        cp = remote(
            region(kind, origin, part), region(kind, origin, part),
            ss.at[4 + kind], gr_sem.at[kind, half, group, slot],
            dev(nbr(axis, up), y, k),
        )
        cp.start()

    def landed(kind, half, group, slot, origin, part):
        cp = remote(
            region(kind, origin, part), region(kind, origin, part),
            ss.at[4 + kind], gr_sem.at[kind, half, group, slot],
            dev(nbr(0, True), y, k),
        )
        cp.wait_recv()

    def whole(half):
        return 4 + half

    def ring_start(kind, half, group, origin, axis):
        hop(kind, half, group, 0, origin, whole(half), axis, True)
        hop(kind, half, group, 1, origin, whole(half), axis, False)

    def ring_relay(kind, half, group, base, axis):
        low, high = shifted(axis, base, 3), shifted(axis, base, 1)
        landed(kind, half, group, 0, low, whole(half))
        hop(kind, half, group, 2, low, 2 * half, axis, True)
        landed(kind, half, group, 1, high, whole(half))
        hop(kind, half, group, 3, high, 2 * half + 1, axis, False)

    def ring_end(kind, half, group, base, axis):
        far = shifted(axis, base, 2)
        landed(kind, half, group, 2, far, 2 * half)
        landed(kind, half, group, 3, far, 2 * half + 1)

    def stage1(kind):
        for half in (0, 1):
            ring_start(kind, half, 0, s, half)
        for half in (0, 1):
            ring_start(kind, half, 1, s, 1 - half)

    def stage2(kind):
        for half in (0, 1):
            ring_relay(kind, half, 0, s, half)
            for g, delta in ((2, 3), (3, 1)):
                ring_start(kind, half, g, shifted(half, s, delta), 1 - half)

    def stage3(kind):
        for half in (0, 1):
            ring_end(kind, half, 0, s, half)
            ring_start(kind, half, 4, shifted(half, s, 2), 1 - half)

    def stage4(kind):
        for g, delta in ((1, 0), (2, 3), (3, 1), (4, 2)):
            for half in (0, 1):
                ring_relay(kind, half, g, shifted(half, s, delta), 1 - half)

    def stage5(kind):
        for g, delta in ((1, 0), (2, 3), (3, 1), (4, 2)):
            for half in (0, 1):
                ring_end(kind, half, g, shifted(half, s, delta), 1 - half)

    load1.wait()
    stage1(0)
    for d in (1, 3, 2):
        yd = (y + d) % 4
        cp = remote(
            prior.at[:, pl.ds(pl.multiple_of(yd * 32, 32), 32), :], prior_r.at[y],
            ss.at[3], sr.at[3], dev(s, yd, k),
        )
        cp.start()

    def send_columns(i, _):
        remote(
            c1p, c1g.at[s], ss.at[0], sr.at[0], dev((s + i) % 16, y, k)
        ).start()
        return 0

    pl.semaphore_wait(rounds.at[0], 3)
    greet(rounds.at[1], z_line)
    lax.fori_loop(1, 16, send_columns, 0)

    all_of(a2.at[pl.ds(1, 3), pl.ds(0, 480)], 2).wait()
    stage1(1)
    stage2(1)
    stage2(0)
    stage3(1)
    stage3(0)
    load3.wait()
    load2.wait()

    pl.semaphore_wait(rounds.at[1], 3)
    greet(rounds.at[2], pair_line)

    all_of(c2g.at[pl.ds(0, 3)], 1).wait()
    all_of(c1g.at[pl.ds(0, 15)], 0).wait()
    cps = [
        pltpu.make_async_copy(c1g, c1s, lsem.at[3]),
        pltpu.make_async_copy(c2g, c2s, lsem.at[4]),
    ]
    for cp in cps:
        cp.start()
    for cp in cps:
        cp.wait()

    stage4(1)
    pl.semaphore_wait(rounds.at[2], 1)
    stage4(0)
    all_of(prior_r.at[pl.ds(0, 3)], 3).wait()

    mask96 = half_lanes((96, 128))
    mask48 = half_lanes((48, 128))

    def forward_state(group):
        return remote(
            xr.at[pl.ds(group * 3, 3), pl.ds(k * 96, 96)],
            xr.at[pl.ds(group * 3, 3), pl.ds(k * 96, 96)],
            ss.at[6], sr.at[6], dev(s, y, 1 - k),
        )

    def state_wait():
        all_of(xr.at[:, pl.ds(pl.multiple_of((1 - k) * 96, 16), 96)], 6).wait()

    macc[...] = jnp.zeros((8, 128), F32)

    def convert(group, _):
        ys = group // 8
        for t in range(3):
            col = pl.multiple_of((group % 8) * 384 + t * 128, 128)
            value = prior_r[ys, :, :, pl.ds(col, 128)].reshape(96, 128)
            macc[...] += jnp.sum(value.reshape(12, 8, 128), axis=0)
            xr[group * 3 + t, pl.ds(pl.multiple_of(k * 96, 16), 96), :] = value.astype(BF)

        @pl.when(group > 0)
        def _():
            forward_state(group - 1).start()

        return 0

    lax.fori_loop(0, 32, convert, 0)
    forward_state(31).start()
    stage5(1)

    def z_places(src_s, src_y, p):
        return (
            (
                pl.ds((src_s * 2 + p) * 3, 3),
                pl.ds(pl.multiple_of(src_y * 32, 32), 32),
                pl.ds(0, 128),
            ),
            (
                p,
                pl.ds(src_s * 3, 3),
                pl.ds(pl.multiple_of(src_y * 16, 16), 16),
                pl.ds(0, 128),
            ),
        )

    ZG = x + 2 * z

    def z_copies(i):
        yd = (y + i * (1 + 2 * k)) % 4
        g = (i // 4 + ZG) % 4
        for d in range(2):
            sd = k * 8 + g * 2 + d
            slot = yd * 8 + g * 2 + d
            for p in range(2):
                self_part = jnp.logical_and(jnp.logical_and(sd == s, yd == y), k == p)
                full_at, packed_at = z_places(s, y, p)
                full = remote(
                    zsend.at[slot, p], zc.at[full_at],
                    ss.at[7], zr_sem.at[s], dev(sd, yd, p),
                )
                packed = remote(
                    zspk.at[slot, :, pl.ds(p * 16, 16), :], zpk.at[packed_at],
                    ss.at[7], zr_sem.at[s], dev(sd, yd, p),
                )

                @pl.when(jnp.logical_not(self_part))
                def _():
                    full.start()
                    packed.start()

                @pl.when(self_part)
                def _():
                    zc[full_at] = zsend[slot, p]
                    zpk[packed_at] = zspk[slot, :, p * 16 : p * 16 + 16, :]

    def z_compute(i, _):
        yd = (y + i * (1 + 2 * k)) % 4
        g = (i // 4 + ZG) % 4
        yr = (i * (1 + 2 * k)) % 4
        values = []
        for t in range(3):
            jl = g * 3 + t
            acc = None
            for slot in range(5):
                c = c2s[yd, k * 12 + jl, slot]
                tile = a2[yr, pl.ds(pl.multiple_of((jl * 5 + slot) * 128, 128), 128), :]
                part = lax.dot_general(xr[c], tile, NT, preferred_element_type=F32)
                acc = part if acc is None else acc + part
            inv = 1.0 / acc[192:193, :]
            values.append(acc[0:192, :] * inv)
        out = yd * 8 + g * 2
        for p in range(2):
            rows = slice(p * 96, p * 96 + 96)
            zsend[out, p] = values[0][rows].astype(BF).reshape(3, 32, 128)
            zsend[out + 1, p] = values[2][rows].astype(BF).reshape(3, 32, 128)
        top, bottom = values[1][0:96], values[1][96:192]
        even = jnp.where(mask96, top, swap(bottom))
        odd = jnp.where(mask96, swap(top), bottom)
        zspk[out] = even.astype(BF).reshape(3, 32, 128)
        zspk[out + 1] = odd.astype(BF).reshape(3, 32, 128)

        @pl.when(i > 0)
        def _():
            z_copies(i - 1)

        return 0

    def z_forward(src_s, p):
        full, packed = pl.ds((src_s * 2 + p) * 3, 3), pl.ds(src_s * 3, 3)
        return [
            remote(ref, ref, ss.at[8], ff_sem.at[src_s], dev(s, y, 1 - k))
            for ref in (zc.at[full, :, pl.ds(0, 128)], zpk.at[p, packed])
        ]

    def z_source(n):
        c = ((s % 8) // 2 + 4 - n // 16) % 4
        r = (n // 4) % 4
        xs = c % 2 + 2 * (r % 2)
        zs = ((c + 4 - xs) // 2) % 2 + 2 * (r // 2)
        return zs * 4 + xs

    def z_receive(i, _):
        src_s = z_source(i * 4)
        own = jnp.logical_and(src_s == s, s // 8 == k)

        @pl.when(own)
        def _():
            rows_of(432, ss.at[7], zr_sem.at[src_s]).wait_recv()

        @pl.when(jnp.logical_not(own))
        def _():
            rows_of(576, ss.at[7], zr_sem.at[src_s]).wait_recv()

        for cp in z_forward(src_s, k):
            cp.start()
        return 0

    def z_finish(i, _):
        rows_of(576, ss.at[8], ff_sem.at[z_source(i * 4)]).wait_recv()
        return 0

    def z_unpack(n, _):
        i = z_source((n // 3) * 4) * 3 + n % 3
        parts = [zpk[p, i].astype(F32).reshape(4, 16, 128) for p in range(2)]
        packed = jnp.concatenate(parts, axis=1).reshape(128, 128)
        lane = lax.broadcasted_iota(jnp.int32, (128, 128), 1)
        fill = jnp.where(lane == 64, 1.0, 0.0).astype(F32)
        block = (i // 3) * 6 + i % 3
        zc[block, :, 128:256] = jnp.where(lane < 64, packed, fill).astype(BF)
        zc[block + 3, :, 128:256] = jnp.where(lane < 64, swap(packed), fill).astype(BF)
        return 0

    def z_complete(i, _):
        z_finish(i, 0)
        for t in range(3):
            z_unpack(i * 3 + t, 0)
        return 0

    def second_stage():
        state_wait()
        lax.fori_loop(0, 16, z_compute, 0)
        z_copies(15)
        for phase in range(5):
            if phase < 4:
                lax.fori_loop(phase * 4, phase * 4 + 4, z_receive, 0)
            if phase > 0:
                lax.fori_loop(phase * 4 - 4, phase * 4, z_complete, 0)

        own = s // 8 == k

        @pl.when(own)
        def _():
            rows_of(32 * 288 - 144, ss.at[7], sr.at[4]).wait_send()

        @pl.when(jnp.logical_not(own))
        def _():
            rows_of(32 * 288, ss.at[7], sr.at[4]).wait_send()

        rows_of(16 * 576, ss.at[8], sr.at[4]).wait_send()

    def partner_at(i, sign):
        j = i // 2
        dz = ((j + 2) % 4) * (1 + 2 * k) * sign
        xa = (x + 2 * ((j // 4 + j) % 2)) % 4
        return ((z + dz) % 4) * 4 + xa + (i % 2) * (1 - 2 * (xa % 2))

    def target(i):
        return partner_at(i, 1)

    def p_copies(i, last):
        sd = target(i)
        if last:
            full = (pfull.at[pl.ds(sd * 3, 3)], outf.at[s])
            packed = (ppk.at[sd], outp.at[s])
            pair = [
                remote(*full, ss.at[9], sr.at[9], dev(sd, y, k)),
                remote(*packed, ss.at[9], sr.at[9], dev(sd, y, k)),
            ]
            mine = [
                pltpu.make_async_copy(*full, lsem.at[5]),
                pltpu.make_async_copy(*packed, lsem.at[6]),
            ]

            @pl.when(sd != s)
            def _():
                for cp in pair:
                    cp.start()

            @pl.when(sd == s)
            def _():
                for cp in mine:
                    cp.start()

            return
        for step in range(4):
            yd = (y + step) % 4
            pair = [
                remote(
                    pfull.at[pl.ds(sd * 3, 3), pl.ds(pl.multiple_of(yd * 32, 32), 32)], prf.at[me],
                    ss.at[9], qr_sem.at[y * 8 + s // 2], dev(sd, yd, k),
                ),
                remote(
                    ppk.at[sd, yd], prp.at[me],
                    ss.at[9], qr_sem.at[y * 8 + s // 2], dev(sd, yd, k),
                ),
            ]

            if step > 0:
                for cp in pair:
                    cp.start()
                continue

            @pl.when(sd != s)
            def _():
                for cp in pair:
                    cp.start()

            @pl.when(sd == s)
            def _():
                prf[me] = pfull[pl.ds(sd * 3, 3), pl.ds(pl.multiple_of(y * 32, 32), 32), :]
                prp[me] = ppk[sd, y]

    def p_compute(last, i, _):
        sd = target(i)
        for t in range(3):
            acc = None
            for slot in range(5):
                c = c1s[sd, t, slot]
                tile = a1[pl.ds(pl.multiple_of((sd * 15 + t * 5 + slot) * 128, 128), 128), :]
                part = lax.dot_general(
                    tile, zc[c], NN, preferred_element_type=F32
                )
                acc = part if acc is None else acc + part
            inv = 1.0 / acc[:, 192:193]
            first = (acc[:, 0:128] * inv).astype(BF)
            second = (acc[:, 128:256] * inv).astype(BF).astype(F32)
            second = jnp.where(half_lanes((128, 128)), second, 0.0)
            total = first.astype(F32) + second
            mpart[...] += jnp.sum(total.reshape(16, 8, 128), axis=0)
            pfull[sd * 3 + t] = first
            ph[t] = second
        for yd in range(4):
            if last:
                flat = ph[...].reshape(384, 128)
                low = flat[yd * 48 : yd * 48 + 48]
                high = flat[192 + yd * 48 : 240 + yd * 48]
            else:
                low = ph[:, yd * 32 : yd * 32 + 16, :].reshape(48, 128)
                high = ph[:, yd * 32 + 16 : yd * 32 + 32, :].reshape(48, 128)
            ppk[sd, yd] = (low + swap(high)).astype(BF)

        @pl.when(jnp.logical_and(i > 0, i <= HELD))
        def _():
            p_copies(i - 1, last)

        return 0

    def first_stage(last, it):
        mpart[...] = jnp.zeros((8, 128), F32)
        lax.fori_loop(0, 16, functools.partial(p_compute, last), 0)
        mine = jnp.sum(MIX * mpart[...] + (1.0 - MIX) * macc[...], axis=0, keepdims=True)
        mbuf[it, me] = mine
        msend[it] = mine

        def total_copy(i, src, dst):
            return remote(
                msend.at[it], mbuf.at[it, src], ss.at[10], sr.at[10], dev(dst // 4, dst % 4, k)
            )

        def total_send(i, _):
            total_copy(i, me, (me + i) % 64).start()
            return 0

        def late(i, _):
            p_copies(i, last)
            return 0

        lax.fori_loop(1, 64, total_send, 0)
        lax.fori_loop(HELD, 16, late, 0)
        all_of(mbuf.at[it, pl.ds(0, 63)], 10).wait()
        mtot[it, 0] = jnp.sum(mbuf[it], axis=0)
        exchange = remote(
            mtot.at[it, 0], mtot.at[it, 1], ss.at[11], sr.at[11], dev(s, y, 1 - k)
        )
        exchange.start()
        exchange.wait()
        grand = jnp.sum(mtot[it, 0] + mtot[it, 1])
        return jnp.full((8, 128), CELLS / grand, F32)

    def p_wait(group):
        own = group == y * 8 + s // 2

        @pl.when(own)
        def _():
            rows_of(144, ss.at[9], qr_sem.at[group]).wait_recv()

        @pl.when(jnp.logical_not(own))
        def _():
            rows_of(288, ss.at[9], qr_sem.at[group]).wait_recv()

    def update_group(n):
        src_s = partner_at((n // 4) * 2, 3)
        return ((y + 4 - n % 4) % 4) * 8 + src_s // 2

    def update(scale, n, _):
        group = update_group(n)
        ys = group // 8
        even = ((group % 8) * 2) * 4 + ys
        odd = even + 4
        p_wait(group)
        a, b = prp[even].astype(F32), prp[odd].astype(F32)
        mid_top = jnp.where(mask48, a, swap(b))
        mid_bottom = jnp.where(mask48, swap(a), b)
        mid = jnp.concatenate(
            [mid_top.reshape(3, 16, 128), mid_bottom.reshape(3, 16, 128)], axis=1
        ).reshape(96, 128)
        first, third = prf[even].astype(F32), prf[odd].astype(F32)
        for t, value in enumerate((first.reshape(96, 128), mid, third.reshape(96, 128))):
            col = pl.multiple_of((group % 8) * 384 + t * 128, 128)
            before = prior_r[ys, :, :, pl.ds(col, 128)].reshape(96, 128)
            now = (MIX * value + (1.0 - MIX) * before) * scale
            xr[group * 3 + t, pl.ds(pl.multiple_of(k * 96, 16), 96), :] = now.astype(BF)

        @pl.when(n > 0)
        def _():
            forward_state(update_group(n - 1)).start()

        return 0

    second_stage()
    stage5(0)
    rows_of(15 * 1920, ss.at[4], sr.at[4]).wait_send()
    rows_of(15 * 1440, ss.at[5], sr.at[4]).wait_send()
    m1 = first_stage(False, 0)
    scale = m1[0:1, :]
    lax.fori_loop(0, 32, functools.partial(update, scale), 0)
    forward_state(update_group(31)).start()

    rows_of(63 * 144, ss.at[9], sr.at[4]).wait_send()

    second_stage()
    mout[...] = first_stage(True, 1)

    rows_of(15 * 576, ss.at[9], sr.at[9]).wait()
    pltpu.make_async_copy(pfull.at[pl.ds(s * 3, 3)], outf.at[s], lsem.at[5]).wait()
    pltpu.make_async_copy(ppk.at[s], outp.at[s], lsem.at[6]).wait()


def run_main(prior, t1, t2, c1, c2):
    any_spec = pl.BlockSpec(memory_space=pl.ANY)
    vmem = pl.BlockSpec(memory_space=pltpu.VMEM)
    dma = pltpu.SemaphoreType.DMA
    scratch = [
        pltpu.VMEM((4, 3, 32, 3072), F32),
        pltpu.VMEM((30720, 128), BF),
        pltpu.VMEM((4, 7680, 128), BF),
        pltpu.VMEM((96, 208, 128), BF),
        pltpu.VMEM((96, 128, 256), BF),
        pltpu.VMEM((2, 48, 64, 128), BF),
        pltpu.VMEM((32, 2, 3, 32, 128), BF),
        pltpu.VMEM((32, 3, 32, 128), BF),
        pltpu.VMEM((48, 128, 128), BF),
        pltpu.VMEM((16, 4, 48, 128), BF),
        pltpu.VMEM((3, 128, 128), F32),
        pltpu.VMEM((64, 3, 32, 128), BF),
        pltpu.VMEM((64, 48, 128), BF),
        pltpu.VMEM((2, 64, 1, 128), F32),
        pltpu.VMEM((2, 1, 128), F32),
        pltpu.VMEM((8, 128), F32),
        pltpu.VMEM((2, 2, 1, 128), F32),
        pltpu.VMEM((8, 128), F32),
        pltpu.VMEM((8, 128), jnp.int32),
        pltpu.VMEM((24, 128), jnp.int32),
        pltpu.VMEM((16, 8, 128), jnp.int32),
        pltpu.VMEM((4, 24, 128), jnp.int32),
        pltpu.SMEM((16, 8, 128), jnp.int32),
        pltpu.SMEM((4, 24, 128), jnp.int32),
        pltpu.SemaphoreType.REGULAR((3,)),
        dma((7,)), dma((12,)), dma((12,)), dma((2, 2, 5, 4)), dma((16,)), dma((16,)), dma((32,)),
    ]
    return pl.pallas_call(
        main_kernel,
        out_shape=(
            jax.ShapeDtypeStruct((16, 3, 128, 128), BF),
            jax.ShapeDtypeStruct((16, 4, 48, 128), BF),
            jax.ShapeDtypeStruct((8, 128), F32),
        ),
        in_specs=[any_spec, any_spec, any_spec, vmem, vmem],
        out_specs=(any_spec, any_spec, vmem),
        scratch_shapes=scratch,
        compiler_params=pltpu.CompilerParams(
            collective_id=0, has_side_effects=True, vmem_limit_bytes=60 << 20
        ),
        name="align",
    )(prior, t1, t2, c1, c2)


def combine_kernel(pf, pp, m, prior, out):
    mask = half_lanes((192, 128))
    scale = m[0:1, :]
    for q in range(CQ):
        cols = pl.ds(q * 384, 384)
        pair = pl.ds(q * 2, 2)
        combine_pair(pf.at[pair], pp.at[pair], scale, mask, prior.at[:, cols], out.at[:, cols])


def combine_pair(pf, pp, scale, mask, prior, out):
    a, b = pp[0].astype(F32), pp[1].astype(F32)
    mid = jnp.concatenate([jnp.where(mask, a, swap(b)), jnp.where(mask, swap(a), b)], axis=0)
    for t, value in enumerate((pf[0].astype(F32), mid, pf[1].astype(F32))):
        cols = slice(t * 128, (t + 1) * 128)
        out[:, cols] = (MIX * value + (1.0 - MIX) * prior[:, cols]) * scale


def combine(pf, pp, m, prior):
    return pl.pallas_call(
        combine_kernel,
        grid=(8 // CQ,),
        out_shape=jax.ShapeDtypeStruct((384, 3072), F32),
        in_specs=[
            pl.BlockSpec((2 * CQ, 384, 128), lambda i: (i, 0, 0)),
            pl.BlockSpec((2 * CQ, 192, 128), lambda i: (i, 0, 0)),
            pl.BlockSpec((8, 128), lambda i: (0, 0)),
            pl.BlockSpec((384, 384 * CQ), lambda i: (0, i)),
        ],
        out_specs=pl.BlockSpec((384, 384 * CQ), lambda i: (0, i)),
        name="combine",
    )(pf, pp, m, prior)


def local(prior_scores, tiles_first, columns_first, tiles_second, columns_second):
    t1 = tiles_first.reshape(1920, 128)
    t2 = tiles_second.reshape(15360, 128)
    pf, pp, m = run_main(
        prior_scores.reshape(3, 128, 3072), t1, t2, columns_first, columns_second
    )
    return combine(
        pf.reshape(16, 384, 128), pp.reshape(16, 192, 128), m, prior_scores
    )


def solution(mesh):
    return jax.shard_map(
        local,
        mesh=mesh,
        in_specs=(
            P("row", "col"),
            P("row", None, None, None),
            P("row", None),
            P("col", None, None, None),
            P("col", None),
        ),
        out_specs=P("row", "col"),
        check_vma=False,
    )
```
